256 devices in a mesh: dp: 64 (over x, z, core), mp: 4 (over y).
Axes of the slice: x: 4, y: 4, z: 8, core: 2. Of those that a mesh axis runs over, the one named last changes fastest.
Arguments:
- hidden_activation: bfloat16 [2, 64, 2, 256, 14336], P(None, 'dp', None, None, 'mp'), may hold values from -6 to 6
- target_head_rows: bfloat16 [2, 64, 2, 256, 4096], P(None, 'dp', None, None, 'mp'), may hold values from -6 to 6
- reference_log_probability: float32 [2, 64, 2, 256], P(None, 'dp'), may hold values from -8 to -0.05
- response_token_mask: int32 [2, 64, 2, 256], P(None, 'dp'), may hold values 0 or 1
- sequence_tile_lengths: int32 [2, 64, 2], P(None, 'dp'), may hold values from 1 to 2
- pair_destination: int32 [2, 64], replicated, may hold values from 0 to 63, each once within a row
- adapter_down_first: bfloat16 [14336, 256], P('mp'), may hold values from -0.046875 to 0.046875
- adapter_down_second: bfloat16 [4096, 256], P('mp'), may hold values from -0.09375 to 0.09375
Outputs:
- pair_margin: float32 [2, 64], P(None, 'dp')
- mean_loss: float32 [], replicated
- grad_a: float32 [14336, 256], P(('mp', 'dp'))
- grad_b: float32 [4096, 256], P(('mp', 'dp'))
The draws below stay inside these ranges and needn't reach their ends.
Inputs may be any that keep to these rules, and one draw needn't show every extreme that they name: Each row of pair_destination is a permutation of 0 to 63.
All inputs are finite; a program needn't handle non-finite values. No bound on the sum of `response_token_mask` on one device may be relied on, other than what follows from the above.
Results may differ from the reference program's by a relative error of at most 0.0029.
Values sent between devices are 32-bit elements; how exact they have to be, the bound alone decides.
No kernel may reach another device: no remote copies, remote signals or barrier semaphores. Data moves between devices by JAX's collectives and lax.ppermute only.
A program may use at most 128 MiB of HBM per device.

```python
import math
import jax
import jax.numpy as jnp
from jax import lax

MODEL_WIDTH = 4096
HIDDEN_UNITS = 14336
ADAPTER_RANK = 256
TILE = 128
TILES = 2
MICRO = 2
SEQ = 256
PAIRS = 64


def with_ends(result, key, low, high):
    place = [jax.random.randint(jax.random.fold_in(key, axis), (), 0, length) for axis, length in enumerate(result.shape)]
    widest = result.shape.index(max(result.shape))
    beside = place[:widest] + [(place[widest] + 1) % result.shape[widest]] + place[widest + 1:]
    return result.at[tuple(place)].set(low).at[tuple(beside)].set(high)


def shard_levels(own_key, dims, split, low, high):
    def one(axis_at, parts):
        draws = jax.random.uniform(jax.random.fold_in(jax.random.fold_in(own_key, 6), axis_at), (parts,), jnp.float32, low / len(split), high / len(split))
        return jnp.repeat(jnp.exp(draws), dims[axis_at] // parts).reshape((-1,) + (1,) * (len(dims) - axis_at - 1))

    loudness = one(*split[0])
    for cut in split[1:]:
        loudness = loudness * one(*cut)
    return loudness


def centred(rng, extent, spread, limit, split=(), dtype=jnp.bfloat16):
    values = spread * jax.random.normal(rng, extent, jnp.float32)
    if split:
        values = values * shard_levels(rng, extent, split, -0.22, 0.18)
    return jnp.clip(values, -limit, limit).astype(dtype)


def setup_inputs(seed: int = 0) -> dict:
    key_list = jax.random.split(jax.random.key(seed), 9)
    hidden_activation = centred(key_list[0], (MICRO, PAIRS, 2, SEQ, HIDDEN_UNITS), 1.0, 6.0, ((1, 64), (4, 4)))
    target_head_rows = centred(key_list[1], (MICRO, PAIRS, 2, SEQ, MODEL_WIDTH), 1.0, 6.0, ((1, 64), (4, 4)))
    reference_log_probability = jnp.clip(-8.0 + 7.95 * jax.random.uniform(key_list[2], (MICRO, PAIRS, 2, SEQ), jnp.float32) ** shard_levels(key_list[2], (MICRO, PAIRS, 2, SEQ), ((1, 64),), -0.2, 0.2), -8.0, -0.05)
    response_token_mask = with_ends((jax.random.randint(key_list[3], (MICRO, PAIRS, 2, SEQ), 0, 4) < 3).astype(jnp.int32), jax.random.fold_in(key_list[3], 1), 0, 1)
    sequence_tile_lengths = with_ends(jax.random.randint(key_list[4], (MICRO, PAIRS, 2), 1, TILES + 1), jax.random.fold_in(key_list[4], 1), 1, TILES).astype(jnp.int32)
    pair_destination = jax.vmap(lambda own: jax.random.permutation(own, PAIRS))(jax.random.split(key_list[5], MICRO)).reshape((MICRO, PAIRS)).astype(jnp.int32)
    adapter_down_first = centred(key_list[6], (HIDDEN_UNITS, ADAPTER_RANK), HIDDEN_UNITS ** -0.5, 0.046875, ((0, 4),))
    adapter_down_second = centred(key_list[7], (MODEL_WIDTH, ADAPTER_RANK), MODEL_WIDTH ** -0.5, 0.09375, ((0, 4),))
    return {"hidden_activation": hidden_activation, "target_head_rows": target_head_rows, "reference_log_probability": reference_log_probability, "response_token_mask": response_token_mask, "sequence_tile_lengths": sequence_tile_lengths, "pair_destination": pair_destination, "adapter_down_first": adapter_down_first, "adapter_down_second": adapter_down_second}


BETA = 0.1

def pair_loss_terms(hidden_pair, rows_pair, ref_pair, mask_pair, length_pair, weight_a, weight_b):
    hidden_flattened = hidden_pair.reshape(-1, hidden_pair.shape[-1])
    rows_flattened = rows_pair.reshape(-1, rows_pair.shape[-1])
    latent = jnp.dot(hidden_flattened, weight_a, preferred_element_type=jnp.float32)
    readout = jnp.dot(rows_flattened, weight_b, preferred_element_type=jnp.float32)
    rank_square_root = math.sqrt(weight_a.shape[1])
    shift = (lax.optimization_barrier(jnp.sum(latent * readout, axis=-1)) / rank_square_root).reshape(ref_pair.shape)
    chance = jnp.exp(ref_pair)
    denom = 1.0 - chance + chance * jnp.exp(shift)
    gain = shift - jnp.log(denom)
    positions = (jnp.arange(ref_pair.shape[-1]) // TILE).astype(jnp.int32)
    live_mask = ((mask_pair == 1) & (positions[None, :] < length_pair[:, None])).astype(jnp.float32)
    seq_sums = lax.optimization_barrier(jnp.sum(live_mask * gain, axis=-1))
    reward_margin = BETA * (seq_sums[0] - seq_sums[1])
    slope = -jax.nn.sigmoid(-reward_margin)
    signs = jnp.array([1.0, -1.0], jnp.float32)
    factor = live_mask * (slope * BETA) * signs[:, None] * (1.0 - chance) / denom / rank_square_root
    factor = factor.reshape(-1, 1)
    d_latent = (factor * readout).astype(jnp.bfloat16)
    d_readout = (factor * latent).astype(jnp.bfloat16)
    contract = (((0,), (0,)), ((), ()))
    first_portion = lax.dot_general(hidden_flattened, d_latent, contract, preferred_element_type=jnp.float32)
    second_portion = lax.dot_general(rows_flattened, d_readout, contract, preferred_element_type=jnp.float32)
    return (reward_margin, first_portion, second_portion)

def reference(hidden_activation, target_head_rows, reference_log_probability, response_token_mask, sequence_tile_lengths, pair_destination, adapter_down_first, adapter_down_second):
    total_pairs = MICRO * PAIRS
    items = (hidden_activation.reshape(total_pairs, 2, SEQ, HIDDEN_UNITS), target_head_rows.reshape(total_pairs, 2, SEQ, MODEL_WIDTH), reference_log_probability.reshape(total_pairs, 2, SEQ), response_token_mask.reshape(total_pairs, 2, SEQ), sequence_tile_lengths.reshape(total_pairs, 2))

    def advance(carry, pair_entry):
        reward_margin, first_portion, second_portion = pair_loss_terms(pair_entry[0], pair_entry[1], pair_entry[2], pair_entry[3], pair_entry[4], adapter_down_first, adapter_down_second)
        return ((carry[0] + first_portion, carry[1] + second_portion), reward_margin)
    start = (jnp.zeros((HIDDEN_UNITS, ADAPTER_RANK), jnp.float32), jnp.zeros((MODEL_WIDTH, ADAPTER_RANK), jnp.float32))
    (raw_a, raw_b), margins = lax.scan(advance, start, items)
    margins = margins.reshape(MICRO, PAIRS)
    row_index = jnp.arange(MICRO).astype(jnp.int32)[:, None]
    pair_margin = jnp.zeros((MICRO, PAIRS), jnp.float32).at[row_index, pair_destination].set(margins)
    mean_loss = jnp.mean(jax.nn.softplus(-margins))
    squared_values = jnp.sum(raw_a * raw_a) + jnp.sum(raw_b * raw_b)
    adapter_scale = 1.0 / jnp.sqrt(squared_values / (HIDDEN_UNITS * ADAPTER_RANK + MODEL_WIDTH * ADAPTER_RANK) + 1e-06)
    return (pair_margin, mean_loss, raw_a * adapter_scale, raw_b * adapter_scale)
```

```python
import math

import jax
import jax.numpy as jnp
from jax import lax
from jax.sharding import Mesh
from jax.sharding import PartitionSpec as P

TILE = 128
X, Z, C, Y = "dp_0", "dp_1", "dp_2", "mp"
DP = (X, Z, C)
MP_DP = (Y, X, Z, C)
BETA = 0.1


def hop(value, axis, step):
    count = lax.axis_size(axis)
    return lax.ppermute(value, axis, [(i, (i + step) % count) for i in range(count)])


def pick(value, index, dim=0):
    return lax.dynamic_index_in_dim(value, index, dim, keepdims=False)


def halfway(length):
    return length // 2 if length < 16 else (length // 2 + 7) // 8 * 8


def ring_reduce(block_at, axis):
    count = lax.axis_size(axis)
    here = lax.axis_index(axis)
    half = count // 2
    far = block_at((here + half) % count)
    cut = halfway(far.shape[0])
    rightward = hop(far[:cut], axis, 1)
    leftward = hop(far[cut:], axis, -1)
    for distance in range(half - 1, 0, -1):
        right = block_at((here + distance) % count)
        left = block_at((here - distance) % count)
        if distance == half - 1:
            right = jnp.concatenate([right[:cut] + rightward, right[cut:]])
            left = jnp.concatenate([left[:cut], left[cut:] + leftward])
        else:
            right = right + rightward
            left = left + leftward
        rightward = hop(right, axis, 1)
        leftward = hop(left, axis, -1)
    return block_at(here) + rightward + leftward


def ring_gather(block, axis):
    cut = halfway(block.shape[0])
    before = hop(block, axis, 1)
    after = hop(block, axis, -1)
    low = hop(before[:cut], axis, 1)
    high = hop(after[cut:], axis, -1)
    return (block, after, jnp.concatenate([low, high]), before)


def total_over(value, axis):
    total = value
    for step in range(1, lax.axis_size(axis)):
        total = total + hop(value, axis, step)
    return total


def per_device(
    hidden_activation,
    target_head_rows,
    reference_log_probability,
    response_token_mask,
    sequence_tile_lengths,
    pair_destination,
    adapter_down_first,
    adapter_down_second,
):
    micro, _, sides, seq, ff = hidden_activation.shape
    width = target_head_rows.shape[-1]
    rank = adapter_down_first.shape[1]
    blocks = micro * sides
    tokens = blocks * seq
    ways = lax.axis_size(Y)
    root = math.sqrt(rank)
    near = lax.axis_index(C)
    mine = lax.axis_index(Y)
    place = lax.axis_index(DP)
    pairs = lax.axis_size(DP)
    contract = (((0,), (0,)), ((), ()))

    hidden = hidden_activation.reshape(tokens, ff)
    rows = target_head_rows.reshape(tokens, width)
    readout_part = jnp.dot(rows, adapter_down_second, preferred_element_type=jnp.float32)
    latent_part = jnp.dot(hidden, adapter_down_first, preferred_element_type=jnp.float32)
    readout_part = readout_part.reshape(ways, tokens // ways, rank)
    latent_part = latent_part.reshape(ways, tokens // ways, rank)

    readout_own = ring_reduce(lambda i: pick(readout_part, i), Y)
    latent_own = ring_reduce(lambda i: pick(latent_part, i), Y)
    shift_own = jnp.sum(latent_own * readout_own, axis=-1) / root

    def placed(parts):
        whole = jnp.zeros((ways,) + parts[0].shape, parts[0].dtype)
        for step, part in enumerate(parts):
            whole = lax.dynamic_update_index_in_dim(whole, part, (mine + step) % ways, 0)
        return whole

    shift = placed([shift_own] + [hop(shift_own, Y, -step) for step in range(1, ways)])
    shift = shift.reshape(micro, sides, seq)

    reference = reference_log_probability[:, 0]
    chance = jnp.exp(reference)
    denom = 1.0 - chance + chance * jnp.exp(shift)
    gain = shift - jnp.log(denom)
    positions = (jnp.arange(seq) // TILE).astype(jnp.int32)
    live = (
        (response_token_mask[:, 0] == 1)
        & (positions[None, None, :] < sequence_tile_lengths[:, 0][:, :, None])
    ).astype(jnp.float32)
    seq_sums = jnp.sum(live * gain, axis=-1)
    margin = BETA * (seq_sums[:, 0] - seq_sums[:, 1])
    slope = -jax.nn.sigmoid(-margin)
    signs = jnp.array([1.0, -1.0], jnp.float32)
    factor = (
        live * (slope * BETA)[:, None, None] * signs[None, :, None] * (1.0 - chance) / denom / root
    ).reshape(ways, tokens // ways)

    def scaled(parts):
        return placed(
            [
                (pick(factor, (mine + step) % ways)[:, None] * part).astype(jnp.bfloat16)
                for step, part in enumerate(parts)
            ]
        ).reshape(tokens, rank)

    d_latent = scaled(ring_gather(readout_own, Y))
    d_readout = scaled(ring_gather(latent_own, Y))
    raw_a = lax.dot_general(hidden, d_latent, contract, preferred_element_type=jnp.float32)
    raw_b = lax.dot_general(rows, d_readout, contract, preferred_element_type=jnp.float32)

    def core_sum(raw):
        parts = raw.reshape(lax.axis_size((X, Z)), lax.axis_size(C), -1, rank)
        own = pick(parts, near, 1) + hop(pick(parts, 1 - near, 1), C, 1)
        return own.reshape(lax.axis_size(X), lax.axis_size(Z), -1, rank)

    sum_a = core_sum(raw_a)
    sum_b = core_sum(raw_b)
    column_a = ring_reduce(lambda i: pick(sum_a, i, 0), X)
    shard_a = ring_reduce(lambda i: pick(column_a, i, 0), Z)
    column_b = ring_reduce(lambda i: pick(sum_b, i, 1), Z)
    shard_b = ring_reduce(lambda i: pick(column_b, i, 0), X)

    squares = jnp.sum(shard_a * shard_a) + jnp.sum(shard_b * shard_b)
    target = pick(pair_destination, place, 1)
    hits = jnp.arange(pairs)[None, :] == target[:, None]
    moved = jnp.where(hits, margin[:, None] / ways, 0.0).reshape(-1)
    loss = jnp.sum(jax.nn.softplus(-margin)) / (micro * pairs * ways)
    small = jnp.concatenate([moved, squares[None], loss[None]])
    small = jnp.pad(small, (0, -small.shape[0] % 128)).reshape(1, -1)
    for axis in (C, Y, X, Z):
        small = total_over(small, axis)
    pair_margin = pick(small[0, : micro * pairs].reshape(micro, pairs), place, 1)[:, None]
    squared = small[0, micro * pairs]
    mean_loss = small[0, micro * pairs + 1]
    count = (ff + width) * ways * rank
    scale = 1.0 / jnp.sqrt(squared / count + 1e-06)
    return (pair_margin, mean_loss, shard_a * scale, shard_b * scale)


def solution(mesh):
    split = Mesh(mesh.devices.reshape(4, 8, 2, mesh.shape["mp"]), (X, Z, C, Y))
    placed = (
        P(None, DP, None, None, Y),
        P(None, DP, None, None, Y),
        P(None, DP, None, None),
        P(None, DP, None, None),
        P(None, DP, None),
        P(),
        P(Y, None),
        P(Y, None),
    )
    return jax.shard_map(
        per_device,
        mesh=split,
        in_specs=placed,
        out_specs=(P(None, DP), P(), P(MP_DP, None), P(MP_DP, None)),
        check_vma=False,
    )
```

```python
import math

import jax
import jax.numpy as jnp
from jax import lax
from jax.experimental import pallas as pl
from jax.experimental.pallas import tpu as pltpu
from jax.sharding import Mesh
from jax.sharding import PartitionSpec as P

TILE = 128
X, Z, C, Y = "dp_0", "dp_1", "dp_2", "mp"
DP = (X, Z, C)
MP_DP = (Y, X, Z, C)
BETA = 0.1


def first(i, c, n):
    return (i + 1 - 2 * ((i + c) % 2)) % n


def second(i, c, n):
    return (i - 1 + 2 * ((i + c) % 2)) % n


def third(i, c, n):
    return (i + 3 - 6 * ((i + c) % 2)) % n


def swap(value, axis, partner):
    n = lax.axis_size(axis)
    axes, flat = ((C, Y), lambda i, c: c * n + i) if axis == Y else ((axis, C), lambda i, c: i * 2 + c)
    pairs = [(flat(i, c), flat(partner(i, c, n), c)) for i in range(n) for c in range(2)]
    return lax.ppermute(value, axes, pairs)


def order_of_four(i, c):
    n = 4
    return [first(i, c, n), (i + 2) % n, i, second(i, c, n)]


def order_of_eight(i, c):
    n = 8

    def group(j):
        k = second(j, c, n)
        return [j, third(j, c, n), k, third(k, c, n)]

    return group(first(i, c, n)) + group(i)


def slots(x, z, c):
    xs = order_of_four(x, c)
    zs = order_of_eight(z, c)
    blocks = jnp.stack([a * 8 + b for a in xs for b in zs]).astype(jnp.int32)
    return jnp.zeros((32,), jnp.int32).at[blocks].set(jnp.arange(32, dtype=jnp.int32))


def backward_kernel(
    info, r0, r1, r23, l0, l1, l23, reference, mask, hidden, rows,
    keep, send, margins,
    r_all, l_all, s_all, d_latent, d_readout, blocks,
):
    step = pl.program_id(0)
    seq = reference.shape[1]
    rank = keep.shape[2]
    root = math.sqrt(rank)

    @pl.when(step == 0)
    def _():
        for k, (r, l) in enumerate(
            ((r0[...], l0[...]), (r1[...], l1[...]), (r23[0], l23[0]), (r23[1], l23[1]))
        ):
            at = info[k]
            r_all[at] = r[:seq]
            l_all[at] = l
            s_all[at] = r[seq : seq + 8]
        tile = lax.broadcasted_iota(jnp.int32, (1, seq), 1) // TILE
        live, share, sums = [], [], []
        for q in range(4):
            shift = s_all[q][0:1]
            chance = jnp.exp(reference[q : q + 1])
            denom = 1.0 - chance + chance * jnp.exp(shift)
            gain = shift - jnp.log(denom)
            on = (mask[q : q + 1] == 1) & (tile < info[8 + q])
            live.append(on.astype(jnp.float32))
            share.append((chance, denom))
            sums.append(jnp.sum(live[q] * gain, axis=1, keepdims=True))
        factors = []
        for m in range(2):
            margin = BETA * (sums[2 * m] - sums[2 * m + 1])
            margins[m : m + 1] = jnp.broadcast_to(margin, (1, 128))
            slope = -jax.nn.sigmoid(-margin)
            for side, sign in enumerate((1.0, -1.0)):
                chance, denom = share[2 * m + side]
                factors.append(
                    live[2 * m + side] * (slope * BETA) * sign * (1.0 - chance) / denom / root
                )
        columns = jnp.concatenate(factors + [jnp.zeros((4, seq), jnp.float32)], axis=0).T
        for q in range(4):
            column = columns[:, q : q + 1]
            d_latent[pl.ds(q * seq, seq)] = (column * r_all[q]).astype(jnp.bfloat16)
            d_readout[pl.ds(q * seq, seq)] = (column * l_all[q]).astype(jnp.bfloat16)

    contract = (((0,), (0,)), ((), ()))
    part_a = lax.dot_general(
        hidden[...], d_latent[...], contract, preferred_element_type=jnp.float32
    )
    part_b = lax.dot_general(
        rows[...], d_readout[...], contract, preferred_element_type=jnp.float32
    )
    tall = part_a.shape[0] // 16
    blocks[:, :tall] = part_a.reshape(16, tall, rank)
    blocks[:, tall:] = part_b.reshape(16, part_b.shape[0] // 16, rank)
    core = info[4]
    for z in range(8):
        keep[info[16 + step * 8 + z]] = blocks[2 * z + core]
        send[info[48 + step * 8 + z]] = blocks[2 * z + 1 - core]


def backward(info, readouts, latents, reference, mask, hidden, rows):
    tokens, ff = hidden.shape
    width = rows.shape[1]
    rank = latents[0].shape[1]
    seq = reference.shape[1]
    tall = (ff + width) // 64
    whole = lambda shape: pl.BlockSpec(shape, lambda i, info: (0,) * len(shape))
    return pl.pallas_call(
        backward_kernel,
        grid_spec=pltpu.PrefetchScalarGridSpec(
            num_scalar_prefetch=1,
            grid=(4,),
            in_specs=[whole(v.shape) for v in (*readouts, *latents, reference, mask)]
            + [
                pl.BlockSpec((tokens, ff // 4), lambda i, info: (0, i)),
                pl.BlockSpec((tokens, width // 4), lambda i, info: (0, i)),
            ],
            out_specs=[whole((32, tall, rank)), whole((32, tall, rank)), whole((8, 128))],
            scratch_shapes=[
                pltpu.VMEM((4, seq, rank), jnp.float32),
                pltpu.VMEM((4, seq, rank), jnp.float32),
                pltpu.VMEM((4, 8, seq), jnp.float32),
                pltpu.VMEM((tokens, rank), jnp.bfloat16),
                pltpu.VMEM((tokens, rank), jnp.bfloat16),
                pltpu.VMEM((16, tall, rank), jnp.float32),
            ],
        ),
        out_shape=[
            jax.ShapeDtypeStruct((32, tall, rank), jnp.float32),
            jax.ShapeDtypeStruct((32, tall, rank), jnp.float32),
            jax.ShapeDtypeStruct((8, 128), jnp.float32),
        ],
        compiler_params=pltpu.CompilerParams(
            dimension_semantics=("arbitrary",), vmem_limit_bytes=50 * 2**20
        ),
        cost_estimate=pl.CostEstimate(
            flops=2 * tokens * (ff + width) * rank,
            bytes_accessed=2 * tokens * (ff + width) + 8 * (ff + width) * rank,
            transcendentals=4096,
        ),
    )(info, *readouts, *latents, reference, mask, hidden, rows)


def per_device(
    hidden_activation,
    target_head_rows,
    reference_log_probability,
    response_token_mask,
    sequence_tile_lengths,
    pair_destination,
    adapter_down_first,
    adapter_down_second,
):
    micro, _, sides, seq, ff = hidden_activation.shape
    width = target_head_rows.shape[-1]
    rank = adapter_down_first.shape[1]
    ways = lax.axis_size(Y)
    tokens = micro * sides * seq
    root = math.sqrt(rank)
    x, z, c, y = (lax.axis_index(axis) for axis in (X, Z, C, Y))
    place = lax.axis_index(DP)
    pairs = lax.axis_size(DP)

    hidden = hidden_activation.reshape(tokens, ff)
    rows = target_head_rows.reshape(tokens, width)
    near, far, mine, late = order_of_four(y, c)

    def own_sum(part):
        part = part.reshape(ways, seq, rank)
        at = lambda i: lax.dynamic_index_in_dim(part, i, 0, keepdims=False)
        came = swap(jnp.stack([at(near), at(far)]), Y, first)
        return at(mine) + came[0] + swap(at(late) + came[1], Y, second)

    readout = own_sum(jnp.dot(rows, adapter_down_second, preferred_element_type=jnp.float32))
    latent = own_sum(jnp.dot(hidden, adapter_down_first, preferred_element_type=jnp.float32))
    shift = jnp.sum(latent * readout, axis=-1) / root
    tagged = jnp.concatenate([readout, jnp.broadcast_to(shift[None], (8, seq))])

    def spread(own):
        other = swap(own, Y, second)
        return own, other, swap(jnp.stack([own, other]), Y, first)

    info = jnp.concatenate(
        [
            jnp.stack([mine, late, near, far, c, c, c, c]).astype(jnp.int32),
            sequence_tile_lengths.reshape(-1).astype(jnp.int32),
            jnp.zeros((4,), jnp.int32),
            slots(x, z, c),
            slots(x, z, 1 - c),
        ]
    )
    keep, send, margins = backward(
        info,
        spread(tagged),
        spread(latent),
        reference_log_probability.reshape(ways, seq),
        response_token_mask.reshape(ways, seq),
        hidden,
        rows,
    )
    margin = margins[:micro, 0]

    came = lax.ppermute(send, C, [(0, 1), (1, 0)])
    half = keep[16:] + came[16:] + swap(keep[:16] + came[:16], X, first)
    half = half[:8] + swap(half[8:], X, second)
    half = half[4:] + swap(half[:4], Z, first)
    half = half[:2] + swap(half[2:], Z, second)
    shard = half[0] + swap(half[1], Z, third)

    squares = jnp.sum(shard * shard)
    target = lax.dynamic_index_in_dim(pair_destination, place, 1, keepdims=False)
    hits = jnp.arange(pairs)[:, None] == target[None, :]
    moved = jnp.where(hits, margin[None, :] / ways, 0.0)
    loss = jnp.sum(jax.nn.softplus(-margin)) / (micro * pairs * ways)
    plain = jnp.broadcast_to(jnp.stack([squares, loss])[None], (pairs, 2))
    small = jnp.concatenate([moved, plain], axis=1)
    small = jnp.broadcast_to(small[:, None], (pairs, ways, micro + 2))
    small = small.reshape(pairs * ways, micro + 2)
    small = lax.all_to_all(small, (X, Z, C, Y), 0, 0, tiled=True).sum(axis=0)
    pair_margin = small[:micro, None]
    squared = small[micro]
    mean_loss = small[micro + 1]
    count = (ff + width) * ways * rank
    scale = 1.0 / jnp.sqrt(squared / count + 1e-06)
    cut = ff // pairs
    return (pair_margin, mean_loss, shard[:cut] * scale, shard[cut:] * scale)


def solution(mesh):
    split = Mesh(mesh.devices.reshape(4, 8, 2, mesh.shape["mp"]), (X, Z, C, Y))
    placed = (
        P(None, DP, None, None, Y),
        P(None, DP, None, None, Y),
        P(None, DP, None, None),
        P(None, DP, None, None),
        P(None, DP, None),
        P(),
        P(Y, None),
        P(Y, None),
    )
    return jax.shard_map(
        per_device,
        mesh=split,
        in_specs=placed,
        out_specs=(P(None, DP), P(), P(MP_DP, None), P(MP_DP, None)),
        check_vma=False,
    )
```

```python
import math

import jax
import jax.numpy as jnp
import numpy as np
from jax import lax
from jax.experimental import pallas as pl
from jax.experimental.pallas import tpu as pltpu
from jax.sharding import Mesh
from jax.sharding import PartitionSpec as P

TILE = 128
X, Z, C, Y = "dp_0", "dp_1", "dp_2", "mp"
DP = (X, Z, C)
MP_DP = (Y, X, Z, C)
BETA = 0.1


def first(i, c, n):
    return (i + 1 - 2 * ((i + c) % 2)) % n


def second(i, c, n):
    return (i - 1 + 2 * ((i + c) % 2)) % n


def third(i, c, n):
    return (i + 3 - 6 * ((i + c) % 2)) % n


def swap(value, axis, partner):
    n = lax.axis_size(axis)
    axes, flat = ((C, Y), lambda i, c: c * n + i) if axis == Y else ((axis, C), lambda i, c: i * 2 + c)
    pairs = [(flat(i, c), flat(partner(i, c, n), c)) for i in range(n) for c in range(2)]
    return lax.ppermute(value, axes, pairs)


def order_of_four(i, c):
    n = 4
    return [first(i, c, n), (i + 2) % n, i, second(i, c, n)]


def order_of_eight(i, c):
    n = 8

    def group(j):
        k = second(j, c, n)
        return [j, third(j, c, n), k, third(k, c, n)]

    return group(first(i, c, n)) + group(i)


def places_of(order):
    return [order.index(i) for i in range(len(order))]


def table():
    rows = []
    for x in range(4):
        for z in range(8):
            for c in range(2):
                for y in range(4):
                    near, far, mine, late = order_of_four(y, c)
                    rows.append(
                        [mine, late, near, far, c, 0, 0, 0]
                        + order_of_eight(z, c)
                        + order_of_eight(z, 1 - c)
                        + places_of(order_of_four(x, c))
                        + places_of(order_of_four(x, 1 - c))
                    )
    return np.array(rows, np.int32)


ORDER_HERE, ORDER_THERE, PLACE_HERE, PLACE_THERE, LENGTHS = 8, 16, 24, 28, 32


def arrange(info, part, blocks, outs):
    tall = part.shape[0] // 16
    blocks[...] = part.reshape(16, tall, part.shape[1])
    core = info[4]
    for side, order in enumerate((ORDER_HERE, ORDER_THERE)):
        which = core if side == 0 else 1 - core
        for p in range(8):
            block = blocks[2 * info[order + p] + which]
            row = 0
            for out, z_dim in outs[side]:
                height = out.shape[-2]
                at = (0, p // 4, 0, p % 4) if z_dim == 1 else (p // 4, 0, 0, p % 4)
                out[at] = block[row : row + height]
                row += height


CONTRACT = (((0,), (0,)), ((), ()))


def first_kernel(
    info, r0, r1, r23, reference, mask, hidden,
    keep_p, keep_q, send_p, send_q, margins, columns,
    r_all, s_all, d_latent, blocks,
):
    seq = reference.shape[1]
    root = math.sqrt(r_all.shape[2])

    @pl.when(pl.program_id(0) == 0)
    def _():
        for k, r in enumerate((r0[...], r1[...], r23[0], r23[1])):
            r_all[info[k]] = r[:seq]
            s_all[info[k]] = r[seq:]
        tile = lax.broadcasted_iota(jnp.int32, (1, seq), 1) // TILE
        live, share, sums = [], [], []
        for q in range(4):
            shift = s_all[q][0:1]
            chance = jnp.exp(reference[q : q + 1])
            denom = 1.0 - chance + chance * jnp.exp(shift)
            gain = shift - jnp.log(denom)
            on = (mask[q : q + 1] == 1) & (tile < info[LENGTHS + q])
            live.append(on.astype(jnp.float32))
            share.append((chance, denom))
            sums.append(jnp.sum(live[q] * gain, axis=1, keepdims=True))
        factors = []
        for m in range(2):
            margin = BETA * (sums[2 * m] - sums[2 * m + 1])
            margins[m : m + 1] = jnp.broadcast_to(margin, (1, 128))
            slope = -jax.nn.sigmoid(-margin)
            for side, sign in enumerate((1.0, -1.0)):
                chance, denom = share[2 * m + side]
                factors.append(
                    live[2 * m + side] * (slope * BETA) * sign * (1.0 - chance) / denom / root
                )
        columns[...] = jnp.concatenate(factors + [jnp.zeros((4, seq), jnp.float32)], axis=0).T
        for q in range(4):
            scaled = columns[:, q : q + 1] * r_all[q]
            d_latent[pl.ds(q * seq, seq)] = scaled.astype(jnp.bfloat16)

    part = lax.dot_general(
        hidden[...], d_latent[...], CONTRACT, preferred_element_type=jnp.float32
    )
    arrange(
        info, part, blocks, (((keep_p, 1), (keep_q, 0)), ((send_p, 1), (send_q, 0)))
    )


def second_kernel(
    info, l0, l1, l23, columns, rows, keep, send, l_all, d_readout, blocks
):
    seq = columns.shape[0]

    @pl.when(pl.program_id(0) == 0)
    def _():
        for k, l in enumerate((l0[...], l1[...], l23[0], l23[1])):
            l_all[info[k]] = l
        for q in range(4):
            scaled = columns[:, q : q + 1] * l_all[q]
            d_readout[pl.ds(q * seq, seq)] = scaled.astype(jnp.bfloat16)

    part = lax.dot_general(
        rows[...], d_readout[...], CONTRACT, preferred_element_type=jnp.float32
    )
    arrange(info, part, blocks, (((keep, 0),), ((send, 0),)))


def whole(value):
    return pl.BlockSpec(value.shape, lambda i, info: (0,) * len(value.shape))


def x_major(rows, rank, places):
    return (
        jax.ShapeDtypeStruct((2, 2, 2, 4, rows, rank), jnp.float32),
        pl.BlockSpec(
            (1, 2, 1, 4, rows, rank),
            lambda i, info: (info[places + i] // 2, 0, info[places + i] % 2, 0, 0, 0),
        ),
    )


def z_major(rows, rank, places):
    return (
        jax.ShapeDtypeStruct((2, 2, 2, 4, rows, rank), jnp.float32),
        pl.BlockSpec(
            (2, 1, 1, 4, rows, rank),
            lambda i, info: (0, info[places + i] // 2, info[places + i] % 2, 0, 0, 0),
        ),
    )


def kernel_call(body, info, wholes, streamed, outs, scratch, rank):
    tokens, wide = streamed.shape
    return pl.pallas_call(
        body,
        grid_spec=pltpu.PrefetchScalarGridSpec(
            num_scalar_prefetch=1,
            grid=(4,),
            in_specs=[whole(v) for v in wholes]
            + [pl.BlockSpec((tokens, wide // 4), lambda i, info: (0, i))],
            out_specs=[spec for _, spec in outs],
            scratch_shapes=scratch,
        ),
        out_shape=[shape for shape, _ in outs],
        compiler_params=pltpu.CompilerParams(
            dimension_semantics=("arbitrary",), vmem_limit_bytes=28 * 2**20
        ),
        cost_estimate=pl.CostEstimate(
            flops=2 * tokens * wide * rank,
            bytes_accessed=2 * tokens * wide + 4 * wide * rank,
            transcendentals=4096,
        ),
    )(info, *wholes, streamed)


def per_device(
    hidden_activation,
    target_head_rows,
    reference_log_probability,
    response_token_mask,
    sequence_tile_lengths,
    pair_destination,
    adapter_down_first,
    adapter_down_second,
):
    micro, _, sides, seq, ff = hidden_activation.shape
    width = target_head_rows.shape[-1]
    rank = adapter_down_first.shape[1]
    ways = lax.axis_size(Y)
    tokens = micro * sides * seq
    root = math.sqrt(rank)
    c, y = lax.axis_index(C), lax.axis_index(Y)
    place = lax.axis_index(DP)
    pairs = lax.axis_size(DP)
    tall_a, tall_b = ff // pairs, width // pairs
    late_a = (tall_a - tall_b) // 16 * 8 if tall_a > 2 * tall_b else tall_a // 2
    late_a = min(late_a, tall_b)

    hidden = hidden_activation.reshape(tokens, ff)
    rows = target_head_rows.reshape(tokens, width)
    near, far, mine, late = order_of_four(y, c)

    def own_sum(part):
        part = part.reshape(ways, seq, rank)
        at = lambda i: lax.dynamic_index_in_dim(part, i, 0, keepdims=False)
        came = swap(jnp.stack([at(near), at(far)]), Y, first)
        return at(mine) + came[0] + swap(at(late) + came[1], Y, second)

    readout_part = jnp.dot(rows, adapter_down_second, preferred_element_type=jnp.float32)
    readout_part, hidden_later = lax.optimization_barrier((readout_part, hidden))
    latent_part = jnp.dot(hidden_later, adapter_down_first, preferred_element_type=jnp.float32)
    readout = own_sum(readout_part)
    latent = own_sum(latent_part)
    shift = jnp.sum(latent * readout, axis=-1) / root
    tagged = jnp.concatenate([readout, jnp.broadcast_to(shift[None], (8, seq))])

    def spread(own):
        other = swap(own, Y, second)
        return own, other, swap(jnp.stack([own, other]), Y, first)

    readouts = spread(tagged)
    latents = spread(latent)

    entry = jnp.asarray(table())[place * ways + y]
    lengths = sequence_tile_lengths.reshape(-1).astype(jnp.int32)
    info = jnp.concatenate([entry, lengths, jnp.zeros((4,), jnp.int32)])
    early = tall_a - late_a
    outs = [
        x_major(early, rank, PLACE_HERE),
        z_major(late_a, rank, PLACE_HERE),
        x_major(early, rank, PLACE_THERE),
        z_major(late_a, rank, PLACE_THERE),
    ]
    for shape in ((8, 128), (seq, 8)):
        block = jax.ShapeDtypeStruct(shape, jnp.float32)
        outs.append((block, whole(block)))
    keep_p, keep_q, send_p, send_q, margins, columns = kernel_call(
        first_kernel,
        info,
        (
            *readouts,
            reference_log_probability.reshape(ways, seq),
            response_token_mask.reshape(ways, seq),
        ),
        hidden,
        outs,
        [
            pltpu.VMEM((4, seq, rank), jnp.float32),
            pltpu.VMEM((4, 8, seq), jnp.float32),
            pltpu.VMEM((tokens, rank), jnp.bfloat16),
            pltpu.VMEM((16, tall_a, rank), jnp.float32),
        ],
        rank,
    )
    margin = margins[:micro, 0]
    core = lambda value: lax.ppermute(value, C, [(0, 1), (1, 0)])
    came_p = core(send_p)
    came_q = core(send_q)
    keep_b, send_b = kernel_call(
        second_kernel,
        info,
        (*latents, columns),
        rows,
        [z_major(tall_b, rank, PLACE_HERE), z_major(tall_b, rank, PLACE_THERE)],
        [
            pltpu.VMEM((4, seq, rank), jnp.float32),
            pltpu.VMEM((tokens, rank), jnp.bfloat16),
            pltpu.VMEM((16, tall_b, rank), jnp.float32),
        ],
        rank,
    )
    came_b = core(send_b)

    p = keep_p[1] + came_p[1] + swap(keep_p[0] + came_p[0], X, first)
    late_rows = lambda i: jnp.concatenate([keep_q[i] + came_q[i], keep_b[i] + came_b[i]], axis=-2)
    w = late_rows(1) + swap(late_rows(0), Z, first)
    p = p[1] + swap(p[0], Z, first)
    w = w[1] + swap(w[0], X, first)
    both = lambda i: jnp.concatenate([p[i], w[i]], axis=-2)
    shard = both(0) + swap(both(1), X, second)
    shard = shard[:2] + swap(shard[2:], Z, second)
    shard = shard[0] + swap(shard[1], Z, third)

    squares = jnp.sum(shard * shard)
    target = lax.dynamic_index_in_dim(pair_destination, place, 1, keepdims=False)
    hits = jnp.arange(pairs)[:, None] == target[None, :]
    moved = jnp.where(hits, margin[None, :] / ways, 0.0)
    loss = jnp.sum(jax.nn.softplus(-margin)) / (micro * pairs * ways)
    plain = jnp.broadcast_to(jnp.stack([squares, loss])[None], (pairs, 2))
    small = jnp.concatenate([moved, plain], axis=1)
    small = jnp.broadcast_to(small[:, None], (pairs, ways, micro + 2))
    small = small.reshape(pairs * ways, micro + 2)
    small = lax.all_to_all(small, (X, Z, C, Y), 0, 0, tiled=True).sum(axis=0)
    pair_margin = small[:micro, None]
    squared = small[micro]
    mean_loss = small[micro + 1]
    count = (ff + width) * ways * rank
    scale = 1.0 / jnp.sqrt(squared / count + 1e-06)
    return (pair_margin, mean_loss, shard[:tall_a] * scale, shard[tall_a:] * scale)


def solution(mesh):
    split = Mesh(mesh.devices.reshape(4, 8, 2, mesh.shape["mp"]), (X, Z, C, Y))
    placed = (
        P(None, DP, None, None, Y),
        P(None, DP, None, None, Y),
        P(None, DP, None, None),
        P(None, DP, None, None),
        P(None, DP, None),
        P(),
        P(Y, None),
        P(Y, None),
    )
    return jax.shard_map(
        per_device,
        mesh=split,
        in_specs=placed,
        out_specs=(P(None, DP), P(), P(MP_DP, None), P(MP_DP, None)),
        check_vma=False,
    )
```

```python
import functools
import math

import jax
import jax.numpy as jnp
import numpy as np
from jax import lax
from jax.experimental import pallas as pl
from jax.experimental.pallas import tpu as pltpu
from jax.sharding import Mesh
from jax.sharding import PartitionSpec as P

TILE = 128
X, Z, C, Y = "dp_0", "dp_1", "dp_2", "mp"
DP = (X, Z, C)
MP_DP = (Y, X, Z, C)
BETA = 0.1


def first(i, c, n):
    return (i + 1 - 2 * ((i + c) % 2)) % n


def second(i, c, n):
    return (i - 1 + 2 * ((i + c) % 2)) % n


def third(i, c, n):
    return (i + 3 - 6 * ((i + c) % 2)) % n


def swap(value, axis, partner):
    n = lax.axis_size(axis)
    axes, flat = ((C, Y), lambda i, c: c * n + i) if axis == Y else ((axis, C), lambda i, c: i * 2 + c)
    pairs = [(flat(i, c), flat(partner(i, c, n), c)) for i in range(n) for c in range(2)]
    return lax.ppermute(value, axes, pairs)


def order_of_four(i, c):
    n = 4
    return [first(i, c, n), (i + 2) % n, i, second(i, c, n)]


def order_of_eight(i, c):
    n = 8

    def group(j):
        k = second(j, c, n)
        return [j, third(j, c, n), k, third(k, c, n)]

    return group(first(i, c, n)) + group(i)


def places_of(order):
    return [order.index(i) for i in range(len(order))]


def table():
    rows = []
    for x in range(4):
        for z in range(8):
            for c in range(2):
                for y in range(4):
                    near, far, mine, late = order_of_four(y, c)
                    rows.append(
                        [mine, late, near, far, c, 0, 0, 0]
                        + order_of_eight(z, c)
                        + order_of_eight(z, 1 - c)
                        + places_of(order_of_four(x, c))
                        + places_of(order_of_four(x, 1 - c))
                    )
    return np.array(rows, np.int32)


ORDER_HERE, ORDER_THERE, PLACE_HERE, PLACE_THERE, LENGTHS = 8, 16, 24, 28, 32


def arrange(info, part, blocks, outs):
    tall = part.shape[0] // 16
    blocks[...] = part.reshape(16, tall, part.shape[1])
    core = info[4]
    for side, order in enumerate((ORDER_HERE, ORDER_THERE)):
        which = core if side == 0 else 1 - core
        for p in range(8):
            block = blocks[2 * info[order + p] + which]
            row = 0
            for out, z_dim in outs[side]:
                height = out.shape[-2]
                at = (0, p // 4, 0, p % 4) if z_dim == 1 else (p // 4, 0, 0, p % 4)
                out[at] = block[row : row + height]
                row += height


CONTRACT = (((0,), (0,)), ((), ()))


def first_kernel(
    info, r0, r1, r2, r3, s0, s1, s2, s3, reference, mask, hidden,
    keep_p, keep_q, send_p, send_q, margins, columns,
    r_all, s_all, d_latent, blocks, tiles, arrived,
):
    seq = reference.shape[1]
    root = math.sqrt(r_all.shape[2])
    step = pl.program_id(0)
    wide = tiles.shape[2]

    def fetch(i):
        slot = i % 2
        at = pl.multiple_of(i * wide, wide)
        return pltpu.make_async_copy(
            hidden.at[:, pl.ds(at, wide)], tiles.at[slot], arrived.at[slot]
        )

    @pl.when(step == 0)
    def _():
        fetch(0).start()
        fetch(1).start()
        for k, (r, s) in enumerate(((r0, s0), (r1, s1), (r2, s2), (r3, s3))):
            r_all[info[k]] = r[...]
            s_all[info[k]] = s[...]
        tile = lax.broadcasted_iota(jnp.int32, (1, seq), 1) // TILE
        live, share, sums = [], [], []
        for q in range(4):
            shift = s_all[q]
            chance = jnp.exp(reference[q : q + 1])
            denom = 1.0 - chance + chance * jnp.exp(shift)
            gain = shift - jnp.log(denom)
            on = (mask[q : q + 1] == 1) & (tile < info[LENGTHS + q])
            live.append(on.astype(jnp.float32))
            share.append((chance, denom))
            sums.append(jnp.sum(live[q] * gain, axis=1, keepdims=True))
        factors = []
        for m in range(2):
            margin = BETA * (sums[2 * m] - sums[2 * m + 1])
            margins[m : m + 1] = jnp.broadcast_to(margin, (1, 128))
            slope = -jax.nn.sigmoid(-margin)
            for side, sign in enumerate((1.0, -1.0)):
                chance, denom = share[2 * m + side]
                factors.append(
                    live[2 * m + side] * (slope * BETA) * sign * (1.0 - chance) / denom / root
                )
        columns[...] = jnp.concatenate(factors + [jnp.zeros((4, seq), jnp.float32)], axis=0).T
        for q in range(4):
            scaled = columns[:, q : q + 1] * r_all[q]
            d_latent[pl.ds(q * seq, seq)] = scaled.astype(jnp.bfloat16)

    fetch(step).wait()
    part = lax.dot_general(
        tiles[step % 2], d_latent[...], CONTRACT, preferred_element_type=jnp.float32
    )
    arrange(
        info, part, blocks, (((keep_p, 1), (keep_q, 0)), ((send_p, 1), (send_q, 0)))
    )

    @pl.when(step < 2)
    def _():
        fetch(step + 2).start()


def second_kernel(
    info, l0, l1, l2, l3, columns, rows, keep, send, l_all, d_readout, blocks
):
    seq = columns.shape[0]

    @pl.when(pl.program_id(0) == 0)
    def _():
        for k, l in enumerate((l0, l1, l2, l3)):
            l_all[info[k]] = l[...]
        for q in range(4):
            scaled = columns[:, q : q + 1] * l_all[q]
            d_readout[pl.ds(q * seq, seq)] = scaled.astype(jnp.bfloat16)

    part = lax.dot_general(
        rows[...], d_readout[...], CONTRACT, preferred_element_type=jnp.float32
    )
    arrange(info, part, blocks, (((keep, 0),), ((send, 0),)))


def product_kernel(at, order, value, weights, out, buffer, arrived):
    seq = out.shape[1]
    copies = [
        pltpu.make_async_copy(
            value.at[pl.ds(pl.multiple_of(order[at + i] * seq, seq), seq)],
            buffer.at[i],
            arrived.at[i],
        )
        for i in range(2)
    ]
    for copy in copies:
        copy.start()
    for i, copy in enumerate(copies):
        copy.wait()
        out[i] = jnp.dot(buffer[i], weights[...], preferred_element_type=jnp.float32)


def product(order, at, value, weights, seq):
    wide, rank = weights.shape
    return pl.pallas_call(
        functools.partial(product_kernel, at),
        in_specs=[
            pl.BlockSpec(memory_space=pltpu.SMEM),
            pl.BlockSpec(memory_space=pltpu.HBM),
            pl.BlockSpec(memory_space=pltpu.VMEM),
        ],
        out_specs=pl.BlockSpec(memory_space=pltpu.VMEM),
        scratch_shapes=[
            pltpu.VMEM((2, seq, wide), value.dtype),
            pltpu.SemaphoreType.DMA((2,)),
        ],
        out_shape=jax.ShapeDtypeStruct((2, seq, rank), jnp.float32),
        compiler_params=pltpu.CompilerParams(vmem_limit_bytes=53 * 2**20),
        cost_estimate=pl.CostEstimate(
            flops=4 * seq * wide * rank,
            bytes_accessed=4 * seq * wide + 2 * wide * rank + 8 * seq * rank,
            transcendentals=0,
        ),
    )(order, value, weights)


def pack_kernel(kept, came, base, shard, small):
    total = kept[...] + came[...]
    shard[...] = total
    column = lax.broadcasted_iota(jnp.int32, small.shape, 1)
    squares = jnp.sum(jnp.sum(total * total, axis=0, keepdims=True), axis=1, keepdims=True)
    small[...] = base[...] + jnp.where(column == 2, squares, 0.0)


def scale_kernel(count, small, shard, grad_a, grad_b, moved, loss):
    total = jnp.sum(small[...], axis=0, keepdims=True)
    scale = 1.0 / jnp.sqrt(total[:, 2:3] / count + 1e-06)
    tall = grad_a.shape[0]
    grad_a[...] = shard[:tall] * scale
    grad_b[...] = shard[tall:] * scale
    moved[0:1] = total[:, 0:1]
    moved[1:2] = total[:, 1:2]
    loss[...] = total[:, 3:4]


def whole(value):
    return pl.BlockSpec(value.shape, lambda i, info: (0,) * len(value.shape))


def x_major(rows, rank, places):
    return (
        jax.ShapeDtypeStruct((2, 2, 2, 4, rows, rank), jnp.float32),
        pl.BlockSpec(
            (1, 2, 1, 4, rows, rank),
            lambda i, info: (info[places + i] // 2, 0, info[places + i] % 2, 0, 0, 0),
        ),
    )


def z_major(rows, rank, places):
    return (
        jax.ShapeDtypeStruct((2, 2, 2, 4, rows, rank), jnp.float32),
        pl.BlockSpec(
            (2, 1, 1, 4, rows, rank),
            lambda i, info: (0, info[places + i] // 2, info[places + i] % 2, 0, 0, 0),
        ),
    )


def kernel_call(body, info, wholes, streamed, outs, scratch, rank, by_hand):
    tokens, wide = streamed.shape
    return pl.pallas_call(
        body,
        grid_spec=pltpu.PrefetchScalarGridSpec(
            num_scalar_prefetch=1,
            grid=(4,),
            in_specs=[whole(v) for v in wholes]
            + [
                pl.BlockSpec(memory_space=pltpu.HBM)
                if by_hand
                else pl.BlockSpec((tokens, wide // 4), lambda i, info: (0, i))
            ],
            out_specs=[spec for _, spec in outs],
            scratch_shapes=scratch,
        ),
        out_shape=[shape for shape, _ in outs],
        compiler_params=pltpu.CompilerParams(
            dimension_semantics=("arbitrary",),
            vmem_limit_bytes=(53 if by_hand else 24) * 2**20,
        ),
        cost_estimate=pl.CostEstimate(
            flops=2 * tokens * wide * rank,
            bytes_accessed=2 * tokens * wide + 4 * wide * rank,
            transcendentals=4096,
        ),
    )(info, *wholes, streamed)


def per_device(
    hidden_activation,
    target_head_rows,
    reference_log_probability,
    response_token_mask,
    sequence_tile_lengths,
    pair_destination,
    adapter_down_first,
    adapter_down_second,
):
    micro, _, sides, seq, ff = hidden_activation.shape
    width = target_head_rows.shape[-1]
    rank = adapter_down_first.shape[1]
    ways = lax.axis_size(Y)
    tokens = micro * sides * seq
    root = math.sqrt(rank)
    c, y = lax.axis_index(C), lax.axis_index(Y)
    place = lax.axis_index(DP)
    pairs = lax.axis_size(DP)
    tall_a, tall_b = ff // pairs, width // pairs
    late_a = (tall_a - tall_b) // 16 * 8 if tall_a > 2 * tall_b else tall_a // 2
    late_a = min(late_a, tall_b)

    hidden = hidden_activation.reshape(tokens, ff)
    rows = target_head_rows.reshape(tokens, width)
    near, far, mine, late = order_of_four(y, c)
    order = jnp.stack([mine, late, near, far]).astype(jnp.int32)

    readout_send = product(order, 2, rows, adapter_down_second, seq)
    readout_send, hidden_next = lax.optimization_barrier((readout_send, hidden))
    latent_send = product(order, 2, hidden_next, adapter_down_first, seq)
    latent_send, rows_next, hidden_next = lax.optimization_barrier((latent_send, rows, hidden))
    readout_keep = product(order, 0, rows_next, adapter_down_second, seq)
    latent_keep = product(order, 0, hidden_next, adapter_down_first, seq)

    def own_sum(send, keep):
        came = swap(send, Y, first)
        relayed = swap(keep[1] + came[1], Y, second)
        return lax.optimization_barrier(keep[0] + came[0] + relayed)

    def spread(own):
        other = swap(own, Y, second)
        beside = swap(own, Y, first)
        return own, other, beside, swap(other, Y, first)

    readout = own_sum(readout_send, readout_keep)
    latent = own_sum(latent_send, latent_keep)
    readouts = spread(readout)
    shift = (jnp.sum(latent * readout, axis=-1) / root)[None]
    opposite = [(i, (i + 2) % 4) for i in range(4)]
    shifts = (shift, swap(shift, Y, second), swap(shift, Y, first), lax.ppermute(shift, Y, opposite))
    latents = spread(latent)

    entry = jnp.asarray(table())[place * ways + y]
    lengths = sequence_tile_lengths.reshape(-1).astype(jnp.int32)
    info = jnp.concatenate([entry, lengths, jnp.zeros((4,), jnp.int32)])
    early = tall_a - late_a
    outs = [
        x_major(early, rank, PLACE_HERE),
        z_major(late_a, rank, PLACE_HERE),
        x_major(early, rank, PLACE_THERE),
        z_major(late_a, rank, PLACE_THERE),
    ]
    for shape in ((8, 128), (seq, 8)):
        block = jax.ShapeDtypeStruct(shape, jnp.float32)
        outs.append((block, whole(block)))
    keep_p, keep_q, send_p, send_q, margins, columns = kernel_call(
        first_kernel,
        info,
        (
            *readouts,
            *shifts,
            reference_log_probability.reshape(ways, seq),
            response_token_mask.reshape(ways, seq),
        ),
        hidden,
        outs,
        [
            pltpu.VMEM((4, seq, rank), jnp.float32),
            pltpu.VMEM((4, 1, seq), jnp.float32),
            pltpu.VMEM((tokens, rank), jnp.bfloat16),
            pltpu.VMEM((16, tall_a, rank), jnp.float32),
            pltpu.VMEM((2, tokens, ff // 4), hidden.dtype),
            pltpu.SemaphoreType.DMA((2,)),
        ],
        rank,
        True,
    )
    margin = margins[:micro, 0]
    core = lambda value: lax.ppermute(value, C, [(0, 1), (1, 0)])
    came_p = core(send_p)
    came_q = core(send_q)
    keep_b, send_b = kernel_call(
        second_kernel,
        info,
        (*latents, columns),
        rows,
        [z_major(tall_b, rank, PLACE_HERE), z_major(tall_b, rank, PLACE_THERE)],
        [
            pltpu.VMEM((4, seq, rank), jnp.float32),
            pltpu.VMEM((tokens, rank), jnp.bfloat16),
            pltpu.VMEM((16, tall_b, rank), jnp.float32),
        ],
        rank,
        False,
    )
    came_b = core(send_b)

    p_send, came_q = lax.optimization_barrier((keep_p[0] + came_p[0], came_q))
    p = swap(p_send, X, first)
    p = keep_p[1] + came_p[1] + p
    late_rows = lambda i: jnp.concatenate([keep_q[i] + came_q[i], keep_b[i] + came_b[i]], axis=-2)
    w = late_rows(1) + swap(late_rows(0), Z, first)
    p = p[1] + swap(p[0], Z, first)
    w = w[1] + swap(w[0], X, first)
    both = lambda i: jnp.concatenate([p[i], w[i]], axis=-2)
    shard = both(0) + swap(both(1), X, second)
    shard = shard[:2] + swap(shard[2:], Z, second)
    kept, came = shard[0], swap(shard[1], Z, third)

    target = lax.dynamic_index_in_dim(pair_destination, place, 1, keepdims=False)
    hits = jnp.arange(pairs)[:, None] == target[None, :]
    moved = jnp.where(hits, margin[None, :] / ways, 0.0)
    loss = jnp.sum(jax.nn.softplus(-margin)) / (micro * pairs * ways)
    plain = jnp.broadcast_to(jnp.stack([jnp.zeros_like(loss), loss])[None], (pairs, 2))
    base = jnp.concatenate([moved, plain], axis=1)
    base = jnp.broadcast_to(base[:, None], (pairs, ways, micro + 2))
    base = base.reshape(pairs * ways, micro + 2)
    little = pltpu.CompilerParams(vmem_limit_bytes=4 * 2**20)
    f32 = lambda *shape: jax.ShapeDtypeStruct(shape, jnp.float32)
    shard, small = pl.pallas_call(
        pack_kernel, out_shape=[f32(*kept.shape), f32(*base.shape)], compiler_params=little
    )(kept, came, base)
    small = lax.all_to_all(small, (X, Z, C, Y), 0, 0, tiled=True)
    grad_a, grad_b, pair_margin, mean_loss = pl.pallas_call(
        functools.partial(scale_kernel, (ff + width) * ways * rank),
        out_shape=[f32(tall_a, rank), f32(tall_b, rank), f32(micro, 1), f32(1, 1)],
        compiler_params=little,
    )(small, shard)
    return (pair_margin, mean_loss[0, 0], grad_a, grad_b)


def solution(mesh):
    split = Mesh(mesh.devices.reshape(4, 8, 2, mesh.shape["mp"]), (X, Z, C, Y))
    placed = (
        P(None, DP, None, None, Y),
        P(None, DP, None, None, Y),
        P(None, DP, None, None),
        P(None, DP, None, None),
        P(None, DP, None),
        P(),
        P(Y, None),
        P(Y, None),
    )

    return jax.shard_map(
        per_device,
        mesh=split,
        in_specs=placed,
        out_specs=(P(None, DP), P(), P(MP_DP, None), P(MP_DP, None)),
        check_vma=False,
    )
```

```python
import functools
import math

import jax
import jax.numpy as jnp
import numpy as np
from jax import lax
from jax.experimental import pallas as pl
from jax.experimental.pallas import tpu as pltpu
from jax.sharding import Mesh
from jax.sharding import PartitionSpec as P

TILE = 128
X, Z, C, Y = "dp_0", "dp_1", "dp_2", "mp"
DP = (X, Z, C)
MP_DP = (Y, X, Z, C)
BETA = 0.1
GRANT_FORWARD, GRANT_BACKWARD = 53, 48


def first(i, c, n):
    return (i + 1 - 2 * ((i + c) % 2)) % n


def second(i, c, n):
    return (i - 1 + 2 * ((i + c) % 2)) % n


def third(i, c, n):
    return (i + 3 - 6 * ((i + c) % 2)) % n


def swap(value, axis, partner):
    n = lax.axis_size(axis)
    axes, flat = ((C, Y), lambda i, c: c * n + i) if axis == Y else ((axis, C), lambda i, c: i * 2 + c)
    pairs = [(flat(i, c), flat(partner(i, c, n), c)) for i in range(n) for c in range(2)]
    return lax.ppermute(value, axes, pairs)


def order_of_four(i, c):
    n = 4
    return [first(i, c, n), (i + 2) % n, i, second(i, c, n)]


def order_of_eight(i, c):
    n = 8

    def group(j):
        k = second(j, c, n)
        return [j, third(j, c, n), k, third(k, c, n)]

    return group(first(i, c, n)) + group(i)


def places_of(order):
    return [order.index(i) for i in range(len(order))]


def table():
    rows = []
    for x in range(4):
        for z in range(8):
            for c in range(2):
                for y in range(4):
                    near, far, mine, late = order_of_four(y, c)
                    rows.append(
                        [mine, late, near, far, c, 0, 0, 0]
                        + order_of_eight(z, c)
                        + order_of_eight(z, 1 - c)
                        + places_of(order_of_four(x, c))
                        + places_of(order_of_four(x, 1 - c))
                    )
    return np.array(rows, np.int32)


ORDER_HERE, ORDER_THERE, PLACE_HERE, PLACE_THERE, LENGTHS = 8, 16, 24, 28, 32


def arrange(info, part, blocks, outs):
    tall = part.shape[0] // 16
    blocks[...] = part.reshape(16, tall, part.shape[1])
    core = info[4]
    for out, order, which in zip(outs, (ORDER_HERE, ORDER_THERE), (core, 1 - core)):
        for p in range(8):
            at = (0, p // 4, 0, p % 4) if out.shape[0] == 1 else (p // 4, 0, 0, p % 4)
            out[at] = blocks[2 * info[order + p] + which]


CONTRACT = (((0,), (0,)), ((), ()))


def first_kernel(
    info, r0, r1, r2, r3, s0, s1, s2, s3, reference, mask, hidden,
    keep_p, send_p, margins, columns,
    r_all, s_all, d_latent, blocks, tiles, arrived,
):
    seq = reference.shape[1]
    root = math.sqrt(r_all.shape[2])
    step = pl.program_id(0)
    wide = tiles.shape[2]

    def fetch(i):
        slot = i % 2
        at = pl.multiple_of(i * wide, wide)
        return pltpu.make_async_copy(
            hidden.at[:, pl.ds(at, wide)], tiles.at[slot], arrived.at[slot]
        )

    @pl.when(step == 0)
    def _():
        fetch(0).start()
        fetch(1).start()
        for k, (r, s) in enumerate(((r0, s0), (r1, s1), (r2, s2), (r3, s3))):
            r_all[info[k]] = r[...]
            s_all[info[k]] = s[...]
        tile = lax.broadcasted_iota(jnp.int32, (1, seq), 1) // TILE
        live, share, sums = [], [], []
        for q in range(4):
            shift = s_all[q]
            chance = jnp.exp(reference[q : q + 1])
            denom = 1.0 - chance + chance * jnp.exp(shift)
            gain = shift - jnp.log(denom)
            on = (mask[q : q + 1] == 1) & (tile < info[LENGTHS + q])
            live.append(on.astype(jnp.float32))
            share.append((chance, denom))
            sums.append(jnp.sum(live[q] * gain, axis=1, keepdims=True))
        factors = []
        for m in range(2):
            margin = BETA * (sums[2 * m] - sums[2 * m + 1])
            margins[m : m + 1] = jnp.broadcast_to(margin, (1, 128))
            slope = -jax.nn.sigmoid(-margin)
            for side, sign in enumerate((1.0, -1.0)):
                chance, denom = share[2 * m + side]
                factors.append(
                    live[2 * m + side] * (slope * BETA) * sign * (1.0 - chance) / denom / root
                )
        columns[...] = jnp.concatenate(factors + [jnp.zeros((4, seq), jnp.float32)], axis=0).T
        for q in range(4):
            scaled = columns[:, q : q + 1] * r_all[q]
            d_latent[pl.ds(q * seq, seq)] = scaled.astype(jnp.bfloat16)

    fetch(step).wait()
    part = lax.dot_general(
        tiles[step % 2], d_latent[...], CONTRACT, preferred_element_type=jnp.float32
    )

    @pl.when(step < 2)
    def _():
        fetch(step + 2).start()

    arrange(info, part, blocks, (keep_p, send_p))


def second_kernel(
    info, l0, l1, l2, l3, columns, rows, keep, send, l_all, d_readout, blocks
):
    seq = columns.shape[0]

    @pl.when(pl.program_id(0) == 0)
    def _():
        for k, l in enumerate((l0, l1, l2, l3)):
            l_all[info[k]] = l[...]
        for q in range(4):
            scaled = columns[:, q : q + 1] * l_all[q]
            d_readout[pl.ds(q * seq, seq)] = scaled.astype(jnp.bfloat16)

    part = lax.dot_general(
        rows[...], d_readout[...], CONTRACT, preferred_element_type=jnp.float32
    )
    arrange(info, part, blocks, (keep, send))


def product_kernel(order, value, weights, send, keep, held, factors, arrived):
    seq = send.shape[1]
    own = pltpu.make_async_copy(weights, factors, arrived.at[4])
    own.start()
    copies = []
    for i in range(4):
        at = pl.ds(pl.multiple_of(order[(i + 2) % 4] * seq, seq), seq)
        copies.append((at, pltpu.make_async_copy(value.at[at], held.at[at], arrived.at[i])))
        copies[i][1].start()
    own.wait()
    for i, (at, copy) in enumerate(copies):
        copy.wait()
        out = send if i < 2 else keep
        out[i % 2] = jnp.dot(held[at], factors[...], preferred_element_type=jnp.float32)


def product(order, value, weights, seq):
    wide, rank = weights.shape
    half = jax.ShapeDtypeStruct((2, seq, rank), jnp.float32)
    return pl.pallas_call(
        product_kernel,
        in_specs=[
            pl.BlockSpec(memory_space=pltpu.SMEM),
            pl.BlockSpec(memory_space=pltpu.HBM),
            pl.BlockSpec(memory_space=pltpu.HBM),
        ],
        out_specs=[pl.BlockSpec(memory_space=pltpu.VMEM)] * 2,
        scratch_shapes=[
            pltpu.VMEM(value.shape, value.dtype),
            pltpu.VMEM(weights.shape, weights.dtype),
            pltpu.SemaphoreType.DMA((5,)),
        ],
        out_shape=[half, half],
        compiler_params=pltpu.CompilerParams(vmem_limit_bytes=GRANT_FORWARD * 2**20),
        cost_estimate=pl.CostEstimate(
            flops=8 * seq * wide * rank,
            bytes_accessed=8 * seq * wide + 2 * wide * rank + 16 * seq * rank,
            transcendentals=0,
        ),
    )(order, value, weights)


def pack_kernel(kept, came, base, shard, small):
    total = kept[...] + came[...]
    shard[...] = total
    column = lax.broadcasted_iota(jnp.int32, small.shape, 1)
    squares = jnp.sum(jnp.sum(total * total, axis=0, keepdims=True), axis=1, keepdims=True)
    small[...] = base[...] + jnp.where(column == 2, squares, 0.0)


def scale_kernel(count, small, shard, grad_a, grad_b, moved, loss):
    total = jnp.sum(small[...], axis=0, keepdims=True)
    scale = 1.0 / jnp.sqrt(total[:, 2:3] / count + 1e-06)
    tall = grad_a.shape[0]
    grad_a[...] = shard[:tall] * scale
    grad_b[...] = shard[tall:] * scale
    moved[0:1] = total[:, 0:1]
    moved[1:2] = total[:, 1:2]
    loss[...] = total[:, 3:4]


def whole(value):
    return pl.BlockSpec(value.shape, lambda i, info: (0,) * len(value.shape))


def x_major(rows, rank, places):
    return (
        jax.ShapeDtypeStruct((2, 2, 2, 4, rows, rank), jnp.float32),
        pl.BlockSpec(
            (1, 2, 1, 4, rows, rank),
            lambda i, info: (info[places + i] // 2, 0, info[places + i] % 2, 0, 0, 0),
        ),
    )


def z_major(rows, rank, places):
    return (
        jax.ShapeDtypeStruct((2, 2, 2, 4, rows, rank), jnp.float32),
        pl.BlockSpec(
            (2, 1, 1, 4, rows, rank),
            lambda i, info: (0, info[places + i] // 2, info[places + i] % 2, 0, 0, 0),
        ),
    )


def kernel_call(body, info, wholes, streamed, outs, scratch, rank, name):
    by_hand = name == "backward_a"
    tokens, wide = streamed.shape
    return pl.pallas_call(
        body,
        grid_spec=pltpu.PrefetchScalarGridSpec(
            num_scalar_prefetch=1,
            grid=(4,),
            in_specs=[whole(v) for v in wholes]
            + [
                pl.BlockSpec(memory_space=pltpu.HBM)
                if by_hand
                else pl.BlockSpec((tokens, wide // 4), lambda i, info: (0, i))
            ],
            out_specs=[spec for _, spec in outs],
            scratch_shapes=scratch,
        ),
        out_shape=[shape for shape, _ in outs],
        compiler_params=pltpu.CompilerParams(
            dimension_semantics=("arbitrary",),
            vmem_limit_bytes=(GRANT_BACKWARD if by_hand else 24) * 2**20,
        ),
        cost_estimate=pl.CostEstimate(
            flops=2 * tokens * wide * rank,
            bytes_accessed=2 * tokens * wide + 4 * wide * rank,
            transcendentals=4096,
        ),
    )(info, *wholes, streamed)


def per_device(
    hidden_activation,
    target_head_rows,
    reference_log_probability,
    response_token_mask,
    sequence_tile_lengths,
    pair_destination,
    adapter_down_first,
    adapter_down_second,
):
    micro, _, sides, seq, ff = hidden_activation.shape
    width = target_head_rows.shape[-1]
    rank = adapter_down_first.shape[1]
    ways = lax.axis_size(Y)
    tokens = micro * sides * seq
    root = math.sqrt(rank)
    c, y = lax.axis_index(C), lax.axis_index(Y)
    place = lax.axis_index(DP)
    pairs = lax.axis_size(DP)
    tall_a, tall_b = ff // pairs, width // pairs

    hidden = hidden_activation.reshape(tokens, ff)
    rows = target_head_rows.reshape(tokens, width)
    near, far, mine, late = order_of_four(y, c)
    order = jnp.stack([mine, late, near, far]).astype(jnp.int32)

    readout_send, readout_keep = product(order, rows, adapter_down_second, seq)
    readout_send, hidden_next = lax.optimization_barrier((readout_send, hidden))
    latent_send, latent_keep = product(order, hidden_next, adapter_down_first, seq)

    def own_sum(send, keep):
        came = swap(send, Y, first)
        relayed = swap(keep[1] + came[1], Y, second)
        return lax.optimization_barrier(keep[0] + came[0] + relayed)

    def spread(own):
        other = swap(own, Y, second)
        beside = swap(own, Y, first)
        return own, other, beside, swap(other, Y, first)

    readout = own_sum(readout_send, readout_keep)
    latent = own_sum(latent_send, latent_keep)
    readouts = spread(readout)
    shift = (jnp.sum(latent * readout, axis=-1) / root)[None]
    opposite = [(i, (i + 2) % 4) for i in range(4)]
    shifts = (shift, swap(shift, Y, second), swap(shift, Y, first), lax.ppermute(shift, Y, opposite))
    latents = spread(latent)

    entry = jnp.asarray(table())[place * ways + y]
    lengths = sequence_tile_lengths.reshape(-1).astype(jnp.int32)
    info = jnp.concatenate([entry, lengths, jnp.zeros((4,), jnp.int32)])
    outs = [x_major(tall_a, rank, PLACE_HERE), x_major(tall_a, rank, PLACE_THERE)]
    for shape in ((8, 128), (seq, 8)):
        block = jax.ShapeDtypeStruct(shape, jnp.float32)
        outs.append((block, whole(block)))
    keep_p, send_p, margins, columns = kernel_call(
        first_kernel,
        info,
        (
            *readouts,
            *shifts,
            reference_log_probability.reshape(ways, seq),
            response_token_mask.reshape(ways, seq),
        ),
        hidden,
        outs,
        [
            pltpu.VMEM((4, seq, rank), jnp.float32),
            pltpu.VMEM((4, 1, seq), jnp.float32),
            pltpu.VMEM((tokens, rank), jnp.bfloat16),
            pltpu.VMEM((16, tall_a, rank), jnp.float32),
            pltpu.VMEM((2, tokens, ff // 4), hidden.dtype),
            pltpu.SemaphoreType.DMA((2,)),
        ],
        rank,
        "backward_a",
    )
    margin = margins[:micro, 0]
    core = lambda value: lax.ppermute(value, C, [(0, 1), (1, 0)])
    came_p = core(send_p)
    keep_b, send_b = kernel_call(
        second_kernel,
        info,
        (*latents, columns),
        rows,
        [z_major(tall_b, rank, PLACE_HERE), z_major(tall_b, rank, PLACE_THERE)],
        [
            pltpu.VMEM((4, seq, rank), jnp.float32),
            pltpu.VMEM((tokens, rank), jnp.bfloat16),
            pltpu.VMEM((16, tall_b, rank), jnp.float32),
        ],
        rank,
        "backward_b",
    )
    came_b = core(send_b)

    p = swap(keep_p[0] + came_p[0], X, first)
    p = keep_p[1] + came_p[1] + p
    w = keep_b[1] + came_b[1] + swap(keep_b[0] + came_b[0], Z, first)
    p = p[1] + swap(p[0], Z, first)
    w = w[1] + swap(w[0], X, first)
    both = lambda i: jnp.concatenate([p[i], w[i]], axis=-2)
    shard = both(0) + swap(both(1), X, second)
    shard = shard[:2] + swap(shard[2:], Z, second)
    kept, came = shard[0], swap(shard[1], Z, third)

    target = lax.dynamic_index_in_dim(pair_destination, place, 1, keepdims=False)
    hits = jnp.arange(pairs)[:, None] == target[None, :]
    moved = jnp.where(hits, margin[None, :] / ways, 0.0)
    loss = jnp.sum(jax.nn.softplus(-margin)) / (micro * pairs * ways)
    plain = jnp.broadcast_to(jnp.stack([jnp.zeros_like(loss), loss])[None], (pairs, 2))
    base = jnp.concatenate([moved, plain], axis=1)
    base = jnp.broadcast_to(base[:, None], (pairs, ways, micro + 2))
    base = base.reshape(pairs * ways, micro + 2)
    little = pltpu.CompilerParams(vmem_limit_bytes=4 * 2**20)
    f32 = lambda *shape: jax.ShapeDtypeStruct(shape, jnp.float32)
    shard, small = pl.pallas_call(
        pack_kernel, out_shape=[f32(*kept.shape), f32(*base.shape)], compiler_params=little
    )(kept, came, base)
    small = lax.all_to_all(small, (X, Z, C, Y), 0, 0, tiled=True)
    grad_a, grad_b, pair_margin, mean_loss = pl.pallas_call(
        functools.partial(scale_kernel, (ff + width) * ways * rank),
        out_shape=[f32(tall_a, rank), f32(tall_b, rank), f32(micro, 1), f32(1, 1)],
        compiler_params=little,
    )(small, shard)
    return (pair_margin, mean_loss[0, 0], grad_a, grad_b)


def solution(mesh):
    split = Mesh(mesh.devices.reshape(4, 8, 2, mesh.shape["mp"]), (X, Z, C, Y))
    placed = (
        P(None, DP, None, None, Y),
        P(None, DP, None, None, Y),
        P(None, DP, None, None),
        P(None, DP, None, None),
        P(None, DP, None),
        P(),
        P(Y, None),
        P(Y, None),
    )

    return jax.shard_map(
        per_device,
        mesh=split,
        in_specs=placed,
        out_specs=(P(None, DP), P(), P(MP_DP, None), P(MP_DP, None)),
        check_vma=False,
    )
```

```python
import functools
import math

import jax
import jax.numpy as jnp
import numpy as np
from jax import lax
from jax.experimental import pallas as pl
from jax.experimental.pallas import tpu as pltpu
from jax.sharding import Mesh
from jax.sharding import PartitionSpec as P

TILE = 128
X, Z, C, Y = "dp_0", "dp_1", "dp_2", "mp"
DP = (X, Z, C)
MP_DP = (Y, X, Z, C)
BETA = 0.1
GRANT_A, GRANT_B = 48, 12


def first(i, c, n):
    return (i + 1 - 2 * ((i + c) % 2)) % n


def second(i, c, n):
    return (i - 1 + 2 * ((i + c) % 2)) % n


def third(i, c, n):
    return (i + 3 - 6 * ((i + c) % 2)) % n


def swap(value, axis, partner):
    n = lax.axis_size(axis)
    axes, flat = ((C, Y), lambda i, c: c * n + i) if axis == Y else ((axis, C), lambda i, c: i * 2 + c)
    pairs = [(flat(i, c), flat(partner(i, c, n), c)) for i in range(n) for c in range(2)]
    return lax.ppermute(value, axes, pairs)


def order_of_four(i, c):
    n = 4
    return [first(i, c, n), (i + 2) % n, i, second(i, c, n)]


def order_of_eight(i, c):
    n = 8

    def group(j):
        k = second(j, c, n)
        return [j, third(j, c, n), k, third(k, c, n)]

    return group(first(i, c, n)) + group(i)


def places_of(order):
    return [order.index(i) for i in range(len(order))]


def table():
    rows = []
    for x in range(4):
        for z in range(8):
            for c in range(2):
                for y in range(4):
                    near, far, mine, late = order_of_four(y, c)
                    rows.append(
                        [mine, late, near, far, c, 0, 0, 0]
                        + order_of_eight(z, c)
                        + order_of_eight(z, 1 - c)
                        + places_of(order_of_four(x, c))
                        + places_of(order_of_four(x, 1 - c))
                    )
    return np.array(rows, np.int32)


ORDER_HERE, ORDER_THERE, PLACE_HERE, PLACE_THERE, LENGTHS = 8, 16, 24, 28, 32


def arrange(info, part, blocks, outs):
    tall = part.shape[0] // 16
    blocks[...] = part.reshape(16, tall, part.shape[1])
    core = info[4]
    for out, order, which in zip(outs, (ORDER_HERE, ORDER_THERE), (core, 1 - core)):
        for p in range(8):
            at = (0, p // 4, 0, p % 4) if out.shape[0] == 1 else (p // 4, 0, 0, p % 4)
            out[at] = blocks[2 * info[order + p] + which]


CONTRACT = (((0,), (0,)), ((), ()))


def first_kernel(
    info, r0, r1, r2, r3, s0, s1, s2, s3, reference, mask, hidden,
    keep_p, send_p, margins, columns,
    r_all, s_all, d_latent, blocks, tiles, arrived,
):
    seq = reference.shape[1]
    root = math.sqrt(r_all.shape[2])
    step = pl.program_id(0)
    wide = tiles.shape[2]

    def fetch(i):
        slot = i % 2
        at = pl.multiple_of(i * wide, wide)
        return pltpu.make_async_copy(
            hidden.at[:, pl.ds(at, wide)], tiles.at[slot], arrived.at[slot]
        )

    @pl.when(step == 0)
    def _():
        fetch(0).start()
        fetch(1).start()
        for k, (r, s) in enumerate(((r0, s0), (r1, s1), (r2, s2), (r3, s3))):
            r_all[info[k]] = r[...]
            s_all[info[k]] = s[...]
        tile = lax.broadcasted_iota(jnp.int32, (1, seq), 1) // TILE
        live, share, sums = [], [], []
        for q in range(4):
            shift = s_all[q]
            chance = jnp.exp(reference[q : q + 1])
            denom = 1.0 - chance + chance * jnp.exp(shift)
            gain = shift - jnp.log(denom)
            on = (mask[q : q + 1] == 1) & (tile < info[LENGTHS + q])
            live.append(on.astype(jnp.float32))
            share.append((chance, denom))
            sums.append(jnp.sum(live[q] * gain, axis=1, keepdims=True))
        factors = []
        for m in range(2):
            margin = BETA * (sums[2 * m] - sums[2 * m + 1])
            margins[m : m + 1] = jnp.broadcast_to(margin, (1, 128))
            slope = -jax.nn.sigmoid(-margin)
            for side, sign in enumerate((1.0, -1.0)):
                chance, denom = share[2 * m + side]
                factors.append(
                    live[2 * m + side] * (slope * BETA) * sign * (1.0 - chance) / denom / root
                )
        columns[...] = jnp.concatenate(factors + [jnp.zeros((4, seq), jnp.float32)], axis=0).T
        for q in range(4):
            scaled = columns[:, q : q + 1] * r_all[q]
            d_latent[pl.ds(q * seq, seq)] = scaled.astype(jnp.bfloat16)

    fetch(step).wait()
    part = lax.dot_general(
        tiles[step % 2], d_latent[...], CONTRACT, preferred_element_type=jnp.float32
    )

    @pl.when(step < 2)
    def _():
        fetch(step + 2).start()

    arrange(info, part, blocks, (keep_p, send_p))


def second_kernel(
    info, l0, l1, l2, l3, columns, rows, keep, send, l_all, d_readout, blocks
):
    seq = columns.shape[0]

    @pl.when(pl.program_id(0) == 0)
    def _():
        for k, l in enumerate((l0, l1, l2, l3)):
            l_all[info[k]] = l[...]
        for q in range(4):
            scaled = columns[:, q : q + 1] * l_all[q]
            d_readout[pl.ds(q * seq, seq)] = scaled.astype(jnp.bfloat16)

    part = lax.dot_general(
        rows[...], d_readout[...], CONTRACT, preferred_element_type=jnp.float32
    )
    arrange(info, part, blocks, (keep, send))


def pack_kernel(kept, other, far, across, base, shard, small):
    total = kept[...] + other[...] + far[...] + across[...]
    shard[...] = total
    column = lax.broadcasted_iota(jnp.int32, small.shape, 1)
    squares = jnp.sum(jnp.sum(total * total, axis=0, keepdims=True), axis=1, keepdims=True)
    small[...] = base[...] + jnp.where(column == 2, squares, 0.0)


def scale_kernel(count, small, shard, grad_a, grad_b, moved, loss):
    total = jnp.sum(small[...], axis=0, keepdims=True)
    scale = 1.0 / jnp.sqrt(total[:, 2:3] / count + 1e-06)
    tall = grad_a.shape[0]
    grad_a[...] = shard[:tall] * scale
    grad_b[...] = shard[tall:] * scale
    moved[0:1] = total[:, 0:1]
    moved[1:2] = total[:, 1:2]
    loss[...] = total[:, 3:4]


def whole(value):
    return pl.BlockSpec(value.shape, lambda i, info: (0,) * len(value.shape))


def x_major(rows, rank, places):
    return (
        jax.ShapeDtypeStruct((2, 2, 2, 4, rows, rank), jnp.float32),
        pl.BlockSpec(
            (1, 2, 1, 4, rows, rank),
            lambda i, info: (info[places + i] // 2, 0, info[places + i] % 2, 0, 0, 0),
        ),
    )


def z_major(rows, rank, places):
    return (
        jax.ShapeDtypeStruct((2, 2, 2, 4, rows, rank), jnp.float32),
        pl.BlockSpec(
            (2, 1, 1, 4, rows, rank),
            lambda i, info: (0, info[places + i] // 2, info[places + i] % 2, 0, 0, 0),
        ),
    )


def kernel_call(body, info, wholes, streamed, outs, scratch, rank, name):
    by_hand = name == "backward_a"
    tokens, wide = streamed.shape
    return pl.pallas_call(
        body,
        grid_spec=pltpu.PrefetchScalarGridSpec(
            num_scalar_prefetch=1,
            grid=(4,),
            in_specs=[whole(v) for v in wholes]
            + [
                pl.BlockSpec(memory_space=pltpu.HBM)
                if by_hand
                else pl.BlockSpec((tokens, wide // 4), lambda i, info: (0, i))
            ],
            out_specs=[spec for _, spec in outs],
            scratch_shapes=scratch,
        ),
        out_shape=[shape for shape, _ in outs],
        compiler_params=pltpu.CompilerParams(
            dimension_semantics=("arbitrary",),
            vmem_limit_bytes=(GRANT_A if by_hand else GRANT_B) * 2**20,
        ),
        cost_estimate=pl.CostEstimate(
            flops=2 * tokens * wide * rank,
            bytes_accessed=2 * tokens * wide + 4 * wide * rank,
            transcendentals=4096,
        ),
    )(info, *wholes, streamed)


def per_device(
    hidden_activation,
    target_head_rows,
    reference_log_probability,
    response_token_mask,
    sequence_tile_lengths,
    pair_destination,
    adapter_down_first,
    adapter_down_second,
):
    micro, _, sides, seq, ff = hidden_activation.shape
    width = target_head_rows.shape[-1]
    rank = adapter_down_first.shape[1]
    ways = lax.axis_size(Y)
    tokens = micro * sides * seq
    root = math.sqrt(rank)
    c, y = lax.axis_index(C), lax.axis_index(Y)
    place = lax.axis_index(DP)
    pairs = lax.axis_size(DP)
    tall_a, tall_b = ff // pairs, width // pairs

    hidden = hidden_activation.reshape(tokens, ff)
    rows = target_head_rows.reshape(tokens, width)
    near, far, mine, late = order_of_four(y, c)

    def product(value, weights):
        return jnp.dot(value, weights, preferred_element_type=jnp.float32).reshape(ways, seq, rank)

    block = lambda part, i: lax.dynamic_index_in_dim(part, i, 0, keepdims=False)
    stacked = lambda part: jnp.stack([block(part, near), block(part, far)])
    readout_part = product(rows, adapter_down_second)
    readout_send, hidden_next = lax.optimization_barrier((stacked(readout_part), hidden))
    latent_part = product(hidden_next, adapter_down_first)
    latent_send = stacked(latent_part)
    readout_keep = [block(readout_part, mine), block(readout_part, late)]
    latent_keep = [block(latent_part, mine), block(latent_part, late)]

    def own_sum(send, keep):
        came = swap(send, Y, first)
        relayed = swap(keep[1] + came[1], Y, second)
        return lax.optimization_barrier(keep[0] + came[0] + relayed)

    def spread(own):
        other = swap(own, Y, second)
        beside = swap(own, Y, first)
        return own, other, beside, swap(other, Y, first)

    readout = own_sum(readout_send, readout_keep)
    latent = own_sum(latent_send, latent_keep)
    readouts = spread(readout)
    shift = (jnp.sum(latent * readout, axis=-1) / root)[None]
    opposite = [(i, (i + 2) % 4) for i in range(4)]
    shift_other = swap(shift, Y, second)
    shift_beside = swap(shift, Y, first)
    shift_far = lax.ppermute(shift, Y, opposite)
    shifts = (shift, shift_other, shift_beside, shift_far)
    latents = spread(latent)

    entry = jnp.asarray(table())[place * ways + y]
    lengths = sequence_tile_lengths.reshape(-1).astype(jnp.int32)
    info = jnp.concatenate([entry, lengths, jnp.zeros((4,), jnp.int32)])
    outs = [x_major(tall_a, rank, PLACE_HERE), x_major(tall_a, rank, PLACE_THERE)]
    for shape in ((8, 128), (seq, 8)):
        block = jax.ShapeDtypeStruct(shape, jnp.float32)
        outs.append((block, whole(block)))
    keep_p, send_p, margins, columns = kernel_call(
        first_kernel,
        info,
        (
            *readouts,
            *shifts,
            reference_log_probability.reshape(ways, seq),
            response_token_mask.reshape(ways, seq),
        ),
        hidden,
        outs,
        [
            pltpu.VMEM((4, seq, rank), jnp.float32),
            pltpu.VMEM((4, 1, seq), jnp.float32),
            pltpu.VMEM((tokens, rank), jnp.bfloat16),
            pltpu.VMEM((16, tall_a, rank), jnp.float32),
            pltpu.VMEM((2, tokens, ff // 4), hidden.dtype),
            pltpu.SemaphoreType.DMA((2,)),
        ],
        rank,
        "backward_a",
    )
    margin = margins[:micro, 0]
    core = lambda value: lax.ppermute(value, C, [(0, 1), (1, 0)])
    came_p = core(send_p)
    keep_b, send_b = kernel_call(
        second_kernel,
        info,
        (*latents, columns),
        rows,
        [z_major(tall_b, rank, PLACE_HERE), z_major(tall_b, rank, PLACE_THERE)],
        [
            pltpu.VMEM((4, seq, rank), jnp.float32),
            pltpu.VMEM((tokens, rank), jnp.bfloat16),
            pltpu.VMEM((16, tall_b, rank), jnp.float32),
        ],
        rank,
        "backward_b",
    )
    came_b = core(send_b)

    p = swap(keep_p[0] + came_p[0], X, first)
    p = keep_p[1] + came_p[1] + p
    w = keep_b[1] + came_b[1] + swap(keep_b[0] + came_b[0], Z, first)
    p = p[1] + swap(p[0], Z, first)
    w = w[1] + swap(w[0], X, first)
    both = lambda i: jnp.concatenate([p[i], w[i]], axis=-2)
    shard = both(0) + swap(both(1), X, second)
    across = lambda i, c, n: third(second(i, c, n), c, n)
    parts = (shard[0],) + tuple(
        swap(shard[k], Z, partner) for k, partner in ((3, across), (1, third), (2, second))
    )

    target = lax.dynamic_index_in_dim(pair_destination, place, 1, keepdims=False)
    hits = jnp.arange(pairs)[:, None] == target[None, :]
    moved = jnp.where(hits, margin[None, :] / ways, 0.0)
    loss = jnp.sum(jax.nn.softplus(-margin)) / (micro * pairs * ways)
    plain = jnp.broadcast_to(jnp.stack([jnp.zeros_like(loss), loss])[None], (pairs, 2))
    base = jnp.concatenate([moved, plain], axis=1)
    base = jnp.broadcast_to(base[:, None], (pairs, ways, micro + 2))
    base = base.reshape(pairs * ways, micro + 2)
    little = pltpu.CompilerParams(vmem_limit_bytes=4 * 2**20)
    f32 = lambda *shape: jax.ShapeDtypeStruct(shape, jnp.float32)
    shard, small = pl.pallas_call(
        pack_kernel, out_shape=[f32(*parts[0].shape), f32(*base.shape)], compiler_params=little
    )(*parts, base)
    small = lax.all_to_all(small, (X, Z, C, Y), 0, 0, tiled=True)
    grad_a, grad_b, pair_margin, mean_loss = pl.pallas_call(
        functools.partial(scale_kernel, (ff + width) * ways * rank),
        out_shape=[f32(tall_a, rank), f32(tall_b, rank), f32(micro, 1), f32(1, 1)],
        compiler_params=little,
    )(small, shard)
    return (pair_margin, mean_loss[0, 0], grad_a, grad_b)


def solution(mesh):
    split = Mesh(mesh.devices.reshape(4, 8, 2, mesh.shape["mp"]), (X, Z, C, Y))
    placed = (
        P(None, DP, None, None, Y),
        P(None, DP, None, None, Y),
        P(None, DP, None, None),
        P(None, DP, None, None),
        P(None, DP, None),
        P(),
        P(Y, None),
        P(Y, None),
    )

    return jax.shard_map(
        per_device,
        mesh=split,
        in_specs=placed,
        out_specs=(P(None, DP), P(), P(MP_DP, None), P(MP_DP, None)),
        check_vma=False,
    )
```

```python
import functools
import math

import jax
import jax.numpy as jnp
import numpy as np
from jax import lax
from jax.experimental import pallas as pl
from jax.experimental.pallas import tpu as pltpu
from jax.sharding import Mesh
from jax.sharding import PartitionSpec as P

TILE = 128
X, Z, C, Y = "dp_0", "dp_1", "dp_2", "mp"
DP = (X, Z, C)
MP_DP = (Y, X, Z, C)
BETA = 0.1
GRANT_A, GRANT_B = 48, 12


def first(i, c, n):
    return (i + 1 - 2 * ((i + c) % 2)) % n


def second(i, c, n):
    return (i - 1 + 2 * ((i + c) % 2)) % n


def third(i, c, n):
    return (i + 3 - 6 * ((i + c) % 2)) % n


def swap(value, axis, partner):
    n = lax.axis_size(axis)
    axes, flat = ((C, Y), lambda i, c: c * n + i) if axis == Y else ((axis, C), lambda i, c: i * 2 + c)
    pairs = [(flat(i, c), flat(partner(i, c, n), c)) for i in range(n) for c in range(2)]
    return lax.ppermute(value, axes, pairs)


def order_of_four(i, c):
    n = 4
    return [first(i, c, n), (i + 2) % n, i, second(i, c, n)]


def order_of_eight(i, c):
    n = 8

    def group(j):
        k = second(j, c, n)
        return [j, third(j, c, n), k, third(k, c, n)]

    return group(first(i, c, n)) + group(i)


def places_of(order):
    return [order.index(i) for i in range(len(order))]


def table():
    rows = []
    for x in range(4):
        for z in range(8):
            for c in range(2):
                for y in range(4):
                    near, far, mine, late = order_of_four(y, c)
                    rows.append(
                        [mine, late, near, far, c, 0, 0, 0]
                        + order_of_eight(z, c)
                        + order_of_eight(z, 1 - c)
                        + places_of(order_of_four(x, c))
                        + places_of(order_of_four(x, 1 - c))
                    )
    return np.array(rows, np.int32)


ORDER_HERE, ORDER_THERE, PLACE_HERE, PLACE_THERE, LENGTHS = 8, 16, 24, 28, 32


def arrange(info, part, blocks, outs):
    tall = part.shape[0] // 16
    blocks[...] = part.reshape(16, tall, part.shape[1])
    core = info[4]
    for out, order, which in zip(outs, (ORDER_HERE, ORDER_THERE), (core, 1 - core)):
        for p in range(8):
            at = (0, p // 4, 0, p % 4) if out.shape[0] == 1 else (p // 4, 0, 0, p % 4)
            out[at] = blocks[2 * info[order + p] + which]


CONTRACT = (((0,), (0,)), ((), ()))


def first_kernel(
    info, r0, r1, r2, r3, s0, s1, s2, s3, reference, mask, hidden,
    keep_p, send_p, margins, columns,
    r_all, s_all, d_latent, blocks, tiles, arrived,
):
    seq = reference.shape[1]
    root = math.sqrt(r_all.shape[2])
    step = pl.program_id(0)
    wide = tiles.shape[2]

    def fetch(i):
        slot = i % 2
        at = pl.multiple_of(i * wide, wide)
        return pltpu.make_async_copy(
            hidden.at[:, pl.ds(at, wide)], tiles.at[slot], arrived.at[slot]
        )

    @pl.when(step == 0)
    def _():
        fetch(0).start()
        fetch(1).start()
        for k, (r, s) in enumerate(((r0, s0), (r1, s1), (r2, s2), (r3, s3))):
            r_all[info[k]] = r[...]
            s_all[info[k]] = s[...]
        tile = lax.broadcasted_iota(jnp.int32, (1, seq), 1) // TILE
        live, share, sums = [], [], []
        for q in range(4):
            shift = s_all[q]
            chance = jnp.exp(reference[q : q + 1])
            denom = 1.0 - chance + chance * jnp.exp(shift)
            gain = shift - jnp.log(denom)
            on = (mask[q : q + 1] == 1) & (tile < info[LENGTHS + q])
            live.append(on.astype(jnp.float32))
            share.append((chance, denom))
            sums.append(jnp.sum(live[q] * gain, axis=1, keepdims=True))
        factors = []
        for m in range(2):
            margin = BETA * (sums[2 * m] - sums[2 * m + 1])
            margins[m : m + 1] = jnp.broadcast_to(margin, (1, 128))
            slope = -jax.nn.sigmoid(-margin)
            for side, sign in enumerate((1.0, -1.0)):
                chance, denom = share[2 * m + side]
                factors.append(
                    live[2 * m + side] * (slope * BETA) * sign * (1.0 - chance) / denom / root
                )
        columns[...] = jnp.concatenate(factors + [jnp.zeros((4, seq), jnp.float32)], axis=0).T
        for q in range(4):
            scaled = columns[:, q : q + 1] * r_all[q]
            d_latent[pl.ds(q * seq, seq)] = scaled.astype(jnp.bfloat16)

    fetch(step).wait()
    part = lax.dot_general(
        tiles[step % 2], d_latent[...], CONTRACT, preferred_element_type=jnp.float32
    )

    @pl.when(step < 2)
    def _():
        fetch(step + 2).start()

    arrange(info, part, blocks, (keep_p, send_p))


def second_kernel(
    info, l0, l1, l2, l3, columns, rows, keep, send, l_all, d_readout, blocks
):
    seq = columns.shape[0]

    @pl.when(pl.program_id(0) == 0)
    def _():
        for k, l in enumerate((l0, l1, l2, l3)):
            l_all[info[k]] = l[...]
        for q in range(4):
            scaled = columns[:, q : q + 1] * l_all[q]
            d_readout[pl.ds(q * seq, seq)] = scaled.astype(jnp.bfloat16)

    part = lax.dot_general(
        rows[...], d_readout[...], CONTRACT, preferred_element_type=jnp.float32
    )
    arrange(info, part, blocks, (keep, send))


def pack_kernel(kept, came, base, shard, small):
    total = kept[...] + came[...]
    shard[...] = total
    column = lax.broadcasted_iota(jnp.int32, small.shape, 1)
    squares = jnp.sum(jnp.sum(total * total, axis=0, keepdims=True), axis=1, keepdims=True)
    small[...] = base[...] + jnp.where(column == 2, squares, 0.0)


def scale_kernel(count, small, shard, grad_a, grad_b, moved, loss):
    total = jnp.sum(small[...], axis=0, keepdims=True)
    scale = 1.0 / jnp.sqrt(total[:, 2:3] / count + 1e-06)
    tall = grad_a.shape[0]
    grad_a[...] = shard[:tall] * scale
    grad_b[...] = shard[tall:] * scale
    moved[0:1] = total[:, 0:1]
    moved[1:2] = total[:, 1:2]
    loss[...] = total[:, 3:4]


def whole(value):
    return pl.BlockSpec(value.shape, lambda i, info: (0,) * len(value.shape))


def x_major(rows, rank, places):
    return (
        jax.ShapeDtypeStruct((2, 2, 2, 4, rows, rank), jnp.float32),
        pl.BlockSpec(
            (1, 2, 1, 4, rows, rank),
            lambda i, info: (info[places + i] // 2, 0, info[places + i] % 2, 0, 0, 0),
        ),
    )


def z_major(rows, rank, places):
    return (
        jax.ShapeDtypeStruct((2, 2, 2, 4, rows, rank), jnp.float32),
        pl.BlockSpec(
            (2, 1, 1, 4, rows, rank),
            lambda i, info: (0, info[places + i] // 2, info[places + i] % 2, 0, 0, 0),
        ),
    )


def kernel_call(body, info, wholes, streamed, outs, scratch, rank, name):
    by_hand = name == "backward_a"
    tokens, wide = streamed.shape
    return pl.pallas_call(
        body,
        grid_spec=pltpu.PrefetchScalarGridSpec(
            num_scalar_prefetch=1,
            grid=(4,),
            in_specs=[whole(v) for v in wholes]
            + [
                pl.BlockSpec(memory_space=pltpu.HBM)
                if by_hand
                else pl.BlockSpec((tokens, wide // 4), lambda i, info: (0, i))
            ],
            out_specs=[spec for _, spec in outs],
            scratch_shapes=scratch,
        ),
        out_shape=[shape for shape, _ in outs],
        compiler_params=pltpu.CompilerParams(
            dimension_semantics=("arbitrary",),
            vmem_limit_bytes=(GRANT_A if by_hand else GRANT_B) * 2**20,
        ),
        cost_estimate=pl.CostEstimate(
            flops=2 * tokens * wide * rank,
            bytes_accessed=2 * tokens * wide + 4 * wide * rank,
            transcendentals=4096,
        ),
    )(info, *wholes, streamed)


def per_device(
    hidden_activation,
    target_head_rows,
    reference_log_probability,
    response_token_mask,
    sequence_tile_lengths,
    pair_destination,
    adapter_down_first,
    adapter_down_second,
):
    micro, _, sides, seq, ff = hidden_activation.shape
    width = target_head_rows.shape[-1]
    rank = adapter_down_first.shape[1]
    ways = lax.axis_size(Y)
    tokens = micro * sides * seq
    root = math.sqrt(rank)
    c, y = lax.axis_index(C), lax.axis_index(Y)
    place = lax.axis_index(DP)
    pairs = lax.axis_size(DP)
    tall_a, tall_b = ff // pairs, width // pairs

    hidden = hidden_activation.reshape(tokens, ff)
    rows = target_head_rows.reshape(tokens, width)
    near, far, mine, late = order_of_four(y, c)

    def product(value, weights):
        return jnp.dot(value, weights, preferred_element_type=jnp.float32).reshape(ways, seq, rank)

    block = lambda part, i: lax.dynamic_index_in_dim(part, i, 0, keepdims=False)
    stacked = lambda part: jnp.stack([block(part, near), block(part, far)])
    readout_part = product(rows, adapter_down_second)
    readout_send, hidden_next = lax.optimization_barrier((stacked(readout_part), hidden))
    latent_part = product(hidden_next, adapter_down_first)
    latent_send = stacked(latent_part)
    readout_keep = [block(readout_part, mine), block(readout_part, late)]
    latent_keep = [block(latent_part, mine), block(latent_part, late)]

    def own_sum(send, keep):
        came = swap(send, Y, first)
        relayed = swap(keep[1] + came[1], Y, second)
        return lax.optimization_barrier(keep[0] + came[0] + relayed)

    def spread(own):
        other = swap(own, Y, second)
        beside = swap(own, Y, first)
        return own, other, beside, swap(other, Y, first)

    readout = own_sum(readout_send, readout_keep)
    latent = own_sum(latent_send, latent_keep)
    readouts = spread(readout)
    shift = (jnp.sum(latent * readout, axis=-1) / root)[None]
    opposite = [(i, (i + 2) % 4) for i in range(4)]
    shift_other = swap(shift, Y, second)
    shift_beside = swap(shift, Y, first)
    shift_far = lax.ppermute(shift, Y, opposite)
    shifts = (shift, shift_other, shift_beside, shift_far)
    latents = spread(latent)

    entry = jnp.asarray(table())[place * ways + y]
    lengths = sequence_tile_lengths.reshape(-1).astype(jnp.int32)
    info = jnp.concatenate([entry, lengths, jnp.zeros((4,), jnp.int32)])
    outs = [x_major(tall_a, rank, PLACE_HERE), x_major(tall_a, rank, PLACE_THERE)]
    for shape in ((8, 128), (seq, 8)):
        block = jax.ShapeDtypeStruct(shape, jnp.float32)
        outs.append((block, whole(block)))
    keep_p, send_p, margins, columns = kernel_call(
        first_kernel,
        info,
        (
            *readouts,
            *shifts,
            reference_log_probability.reshape(ways, seq),
            response_token_mask.reshape(ways, seq),
        ),
        hidden,
        outs,
        [
            pltpu.VMEM((4, seq, rank), jnp.float32),
            pltpu.VMEM((4, 1, seq), jnp.float32),
            pltpu.VMEM((tokens, rank), jnp.bfloat16),
            pltpu.VMEM((16, tall_a, rank), jnp.float32),
            pltpu.VMEM((2, tokens, ff // 4), hidden.dtype),
            pltpu.SemaphoreType.DMA((2,)),
        ],
        rank,
        "backward_a",
    )
    margin = margins[:micro, 0]
    core = lambda value: lax.ppermute(value, C, [(0, 1), (1, 0)])
    came_p = core(send_p)
    keep_b, send_b = kernel_call(
        second_kernel,
        info,
        (*latents, columns),
        rows,
        [z_major(tall_b, rank, PLACE_HERE), z_major(tall_b, rank, PLACE_THERE)],
        [
            pltpu.VMEM((4, seq, rank), jnp.float32),
            pltpu.VMEM((tokens, rank), jnp.bfloat16),
            pltpu.VMEM((16, tall_b, rank), jnp.float32),
        ],
        rank,
        "backward_b",
    )
    came_b = core(send_b)

    def step_on(parts, axis, partner, k=0):
        leaving = functools.reduce(jnp.add, [part[k] for part in parts])
        rest = [part[1 - k] for part in parts]
        leaving, *rest = lax.optimization_barrier((leaving, *rest))
        return [*rest, swap(leaving, axis, partner)]

    p = step_on([keep_p, came_p], X, first)
    w = step_on([keep_b, came_b], Z, first)
    p = step_on(p, Z, first)
    w = step_on(w, X, first)

    def both(k):
        p_sum, w_sum = (functools.reduce(jnp.add, [part[k] for part in parts]) for parts in (p, w))
        return jnp.concatenate([p_sum, w_sum], axis=-2)

    leaving, *rest = lax.optimization_barrier((both(1), *p, *w))
    p, w = rest[: len(p)], rest[len(p) :]
    came = swap(leaving, X, second)
    shard = both(0) + came
    shard = shard[:2] + swap(shard[2:], Z, second)
    parts = (shard[0], swap(shard[1], Z, third))

    target = lax.dynamic_index_in_dim(pair_destination, place, 1, keepdims=False)
    hits = jnp.arange(pairs)[:, None] == target[None, :]
    moved = jnp.where(hits, margin[None, :] / ways, 0.0)
    loss = jnp.sum(jax.nn.softplus(-margin)) / (micro * pairs * ways)
    plain = jnp.broadcast_to(jnp.stack([jnp.zeros_like(loss), loss])[None], (pairs, 2))
    base = jnp.concatenate([moved, plain], axis=1)
    base = jnp.broadcast_to(base[:, None], (pairs, ways, micro + 2))
    base = base.reshape(pairs * ways, micro + 2)
    little = pltpu.CompilerParams(vmem_limit_bytes=4 * 2**20)
    f32 = lambda *shape: jax.ShapeDtypeStruct(shape, jnp.float32)
    shard, small = pl.pallas_call(
        pack_kernel, out_shape=[f32(*parts[0].shape), f32(*base.shape)], compiler_params=little
    )(*parts, base)
    small = lax.all_to_all(small, (X, Z, C, Y), 0, 0, tiled=True)
    grad_a, grad_b, pair_margin, mean_loss = pl.pallas_call(
        functools.partial(scale_kernel, (ff + width) * ways * rank),
        out_shape=[f32(tall_a, rank), f32(tall_b, rank), f32(micro, 1), f32(1, 1)],
        compiler_params=little,
    )(small, shard)
    return (pair_margin, mean_loss[0, 0], grad_a, grad_b)


def solution(mesh):
    split = Mesh(mesh.devices.reshape(4, 8, 2, mesh.shape["mp"]), (X, Z, C, Y))
    placed = (
        P(None, DP, None, None, Y),
        P(None, DP, None, None, Y),
        P(None, DP, None, None),
        P(None, DP, None, None),
        P(None, DP, None),
        P(),
        P(Y, None),
        P(Y, None),
    )

    return jax.shard_map(
        per_device,
        mesh=split,
        in_specs=placed,
        out_specs=(P(None, DP), P(), P(MP_DP, None), P(MP_DP, None)),
        check_vma=False,
    )
```

```python
import functools
import math

import jax
import jax.numpy as jnp
import numpy as np
from jax import lax
from jax.experimental import pallas as pl
from jax.experimental.pallas import tpu as pltpu
from jax.sharding import Mesh
from jax.sharding import PartitionSpec as P

TILE = 128
X, Z, C, Y = "dp_0", "dp_1", "dp_2", "mp"
DP = (X, Z, C)
MP_DP = (Y, X, Z, C)
BETA = 0.1
GRANT_A, GRANT_B = 48, 12


def first(i, c, n):
    return (i + 1 - 2 * ((i + c) % 2)) % n


def second(i, c, n):
    return (i - 1 + 2 * ((i + c) % 2)) % n


def third(i, c, n):
    return (i + 3 - 6 * ((i + c) % 2)) % n


def swap(value, axis, partner):
    n = lax.axis_size(axis)
    axes, flat = ((C, Y), lambda i, c: c * n + i) if axis == Y else ((axis, C), lambda i, c: i * 2 + c)
    pairs = [(flat(i, c), flat(partner(i, c, n), c)) for i in range(n) for c in range(2)]
    return lax.ppermute(value, axes, pairs)


def order_of_four(i, c):
    n = 4
    return [first(i, c, n), (i + 2) % n, i, second(i, c, n)]


def order_of_eight(i, c):
    n = 8

    def group(j):
        k = second(j, c, n)
        return [j, third(j, c, n), k, third(k, c, n)]

    return group(first(i, c, n)) + group(i)


def places_of(order):
    return [order.index(i) for i in range(len(order))]


def table():
    rows = []
    for x in range(4):
        for z in range(8):
            for c in range(2):
                for y in range(4):
                    near, far, mine, late = order_of_four(y, c)
                    rows.append(
                        [mine, late, near, far, c, 0, 0, 0]
                        + order_of_eight(z, c)
                        + order_of_eight(z, 1 - c)
                        + places_of(order_of_four(x, c))
                        + places_of(order_of_four(x, 1 - c))
                    )
    return np.array(rows, np.int32)


ORDER_HERE, ORDER_THERE, PLACE_HERE, PLACE_THERE, LENGTHS = 8, 16, 24, 28, 32


def arrange(info, part, blocks, outs):
    tall = part.shape[0] // 16
    blocks[...] = part.reshape(16, tall, part.shape[1])
    core = info[4]
    for out, order, which in zip(outs, (ORDER_HERE, ORDER_THERE), (core, 1 - core)):
        for p in range(8):
            at = (0, p // 4, 0, p % 4) if out.shape[0] == 1 else (p // 4, 0, 0, p % 4)
            out[at] = blocks[2 * info[order + p] + which]


CONTRACT = (((0,), (0,)), ((), ()))


def first_kernel(
    info, r0, r1, r2, r3, s0, s1, s2, s3, reference, mask, hidden,
    keep_p, send_p, margins, columns,
    r_all, s_all, d_latent, blocks, tiles, arrived,
):
    seq = reference.shape[1]
    root = math.sqrt(r_all.shape[2])
    step = pl.program_id(0)
    wide = tiles.shape[2]

    def fetch(i):
        slot = i % 2
        at = pl.multiple_of(i * wide, wide)
        return pltpu.make_async_copy(
            hidden.at[:, pl.ds(at, wide)], tiles.at[slot], arrived.at[slot]
        )

    @pl.when(step == 0)
    def _():
        fetch(0).start()
        fetch(1).start()
        for k, (r, s) in enumerate(((r0, s0), (r1, s1), (r2, s2), (r3, s3))):
            r_all[info[k]] = r[...]
            s_all[info[k]] = s[...]
        tile = lax.broadcasted_iota(jnp.int32, (1, seq), 1) // TILE
        live, share, sums = [], [], []
        for q in range(4):
            shift = s_all[q]
            chance = jnp.exp(reference[q : q + 1])
            denom = 1.0 - chance + chance * jnp.exp(shift)
            gain = shift - jnp.log(denom)
            on = (mask[q : q + 1] == 1) & (tile < info[LENGTHS + q])
            live.append(on.astype(jnp.float32))
            share.append((chance, denom))
            sums.append(jnp.sum(live[q] * gain, axis=1, keepdims=True))
        factors = []
        for m in range(2):
            margin = BETA * (sums[2 * m] - sums[2 * m + 1])
            margins[m : m + 1] = jnp.broadcast_to(margin, (1, 128))
            slope = -jax.nn.sigmoid(-margin)
            for side, sign in enumerate((1.0, -1.0)):
                chance, denom = share[2 * m + side]
                factors.append(
                    live[2 * m + side] * (slope * BETA) * sign * (1.0 - chance) / denom / root
                )
        columns[...] = jnp.concatenate(factors + [jnp.zeros((4, seq), jnp.float32)], axis=0).T
        for q in range(4):
            scaled = columns[:, q : q + 1] * r_all[q]
            d_latent[pl.ds(q * seq, seq)] = scaled.astype(jnp.bfloat16)

    fetch(step).wait()
    part = lax.dot_general(
        tiles[step % 2], d_latent[...], CONTRACT, preferred_element_type=jnp.float32
    )

    @pl.when(step < 2)
    def _():
        fetch(step + 2).start()

    arrange(info, part, blocks, (keep_p, send_p))


def second_kernel(
    info, l0, l1, l2, l3, columns, rows, keep, send, l_all, d_readout, blocks
):
    seq = columns.shape[0]

    @pl.when(pl.program_id(0) == 0)
    def _():
        for k, l in enumerate((l0, l1, l2, l3)):
            l_all[info[k]] = l[...]
        for q in range(4):
            scaled = columns[:, q : q + 1] * l_all[q]
            d_readout[pl.ds(q * seq, seq)] = scaled.astype(jnp.bfloat16)

    part = lax.dot_general(
        rows[...], d_readout[...], CONTRACT, preferred_element_type=jnp.float32
    )
    arrange(info, part, blocks, (keep, send))


def pack_kernel(kept, came, base, shard, small):
    total = kept[...] + came[...]
    shard[...] = total
    column = lax.broadcasted_iota(jnp.int32, small.shape, 1)
    squares = jnp.sum(jnp.sum(total * total, axis=0, keepdims=True), axis=1, keepdims=True)
    small[...] = base[...] + jnp.where(column == 2, squares, 0.0)


def scale_kernel(count, small, shard, grad_a, grad_b, moved, loss):
    total = jnp.sum(small[...], axis=0, keepdims=True)
    scale = 1.0 / jnp.sqrt(total[:, 2:3] / count + 1e-06)
    tall = grad_a.shape[0]
    grad_a[...] = shard[:tall] * scale
    grad_b[...] = shard[tall:] * scale
    moved[0:1] = total[:, 0:1]
    moved[1:2] = total[:, 1:2]
    loss[...] = total[:, 3:4]


def whole(value):
    return pl.BlockSpec(value.shape, lambda i, info: (0,) * len(value.shape))


def x_major(rows, rank, places):
    return (
        jax.ShapeDtypeStruct((2, 2, 2, 4, rows, rank), jnp.float32),
        pl.BlockSpec(
            (1, 2, 1, 4, rows, rank),
            lambda i, info: (info[places + i] // 2, 0, info[places + i] % 2, 0, 0, 0),
        ),
    )


def z_major(rows, rank, places):
    return (
        jax.ShapeDtypeStruct((2, 2, 2, 4, rows, rank), jnp.float32),
        pl.BlockSpec(
            (2, 1, 1, 4, rows, rank),
            lambda i, info: (0, info[places + i] // 2, info[places + i] % 2, 0, 0, 0),
        ),
    )


def kernel_call(body, info, wholes, streamed, outs, scratch, rank, name):
    by_hand = name == "backward_a"
    tokens, wide = streamed.shape
    return pl.pallas_call(
        body,
        grid_spec=pltpu.PrefetchScalarGridSpec(
            num_scalar_prefetch=1,
            grid=(4,),
            in_specs=[whole(v) for v in wholes]
            + [
                pl.BlockSpec(memory_space=pltpu.HBM)
                if by_hand
                else pl.BlockSpec((tokens, wide // 4), lambda i, info: (0, i))
            ],
            out_specs=[spec for _, spec in outs],
            scratch_shapes=scratch,
        ),
        out_shape=[shape for shape, _ in outs],
        compiler_params=pltpu.CompilerParams(
            dimension_semantics=("arbitrary",),
            vmem_limit_bytes=(GRANT_A if by_hand else GRANT_B) * 2**20,
        ),
        cost_estimate=pl.CostEstimate(
            flops=2 * tokens * wide * rank,
            bytes_accessed=2 * tokens * wide + 4 * wide * rank,
            transcendentals=4096,
        ),
    )(info, *wholes, streamed)


def per_device(
    hidden_activation,
    target_head_rows,
    reference_log_probability,
    response_token_mask,
    sequence_tile_lengths,
    pair_destination,
    adapter_down_first,
    adapter_down_second,
):
    micro, _, sides, seq, ff = hidden_activation.shape
    width = target_head_rows.shape[-1]
    rank = adapter_down_first.shape[1]
    ways = lax.axis_size(Y)
    tokens = micro * sides * seq
    root = math.sqrt(rank)
    c, y = lax.axis_index(C), lax.axis_index(Y)
    place = lax.axis_index(DP)
    pairs = lax.axis_size(DP)
    tall_a, tall_b = ff // pairs, width // pairs

    hidden = hidden_activation.reshape(tokens, ff)
    rows = target_head_rows.reshape(tokens, width)
    near, far, mine, late = order_of_four(y, c)

    def product(value, weights):
        return jnp.dot(value, weights, preferred_element_type=jnp.float32).reshape(ways, seq, rank)

    block = lambda part, i: lax.dynamic_index_in_dim(part, i, 0, keepdims=False)
    stacked = lambda part: jnp.stack([block(part, near), block(part, far)])
    readout_part = product(rows, adapter_down_second)
    readout_send, hidden_next = lax.optimization_barrier((stacked(readout_part), hidden))
    latent_part = product(hidden_next, adapter_down_first)
    latent_send = stacked(latent_part)
    readout_keep = [block(readout_part, mine), block(readout_part, late)]
    latent_keep = [block(latent_part, mine), block(latent_part, late)]

    def own_sum(send, keep):
        came = swap(send, Y, first)
        relayed = swap(keep[1] + came[1], Y, second)
        return lax.optimization_barrier(keep[0] + came[0] + relayed)

    def spread(own):
        other = swap(own, Y, second)
        beside = swap(own, Y, first)
        return own, other, beside, swap(other, Y, first)

    readout = own_sum(readout_send, readout_keep)
    latent = own_sum(latent_send, latent_keep)
    readouts = spread(readout)
    shift = (jnp.sum(latent * readout, axis=-1) / root)[None]
    opposite = [(i, (i + 2) % 4) for i in range(4)]
    shift_other = swap(shift, Y, second)
    shift_beside = swap(shift, Y, first)
    shift_far = lax.ppermute(shift, Y, opposite)
    shifts = (shift, shift_other, shift_beside, shift_far)
    latents = spread(latent)

    entry = jnp.asarray(table())[place * ways + y]
    lengths = sequence_tile_lengths.reshape(-1).astype(jnp.int32)
    info = jnp.concatenate([entry, lengths, jnp.zeros((4,), jnp.int32)])
    outs = [x_major(tall_a, rank, PLACE_HERE), x_major(tall_a, rank, PLACE_THERE)]
    for shape in ((8, 128), (seq, 8)):
        block = jax.ShapeDtypeStruct(shape, jnp.float32)
        outs.append((block, whole(block)))
    keep_p, send_p, margins, columns = kernel_call(
        first_kernel,
        info,
        (
            *readouts,
            *shifts,
            reference_log_probability.reshape(ways, seq),
            response_token_mask.reshape(ways, seq),
        ),
        hidden,
        outs,
        [
            pltpu.VMEM((4, seq, rank), jnp.float32),
            pltpu.VMEM((4, 1, seq), jnp.float32),
            pltpu.VMEM((tokens, rank), jnp.bfloat16),
            pltpu.VMEM((16, tall_a, rank), jnp.float32),
            pltpu.VMEM((2, tokens, ff // 4), hidden.dtype),
            pltpu.SemaphoreType.DMA((2,)),
        ],
        rank,
        "backward_a",
    )
    margin = margins[:micro, 0]
    core = lambda value: lax.ppermute(value, C, [(0, 1), (1, 0)])
    came_p = core(send_p)
    keep_b, send_b = kernel_call(
        second_kernel,
        info,
        (*latents, columns),
        rows,
        [z_major(tall_b, rank, PLACE_HERE), z_major(tall_b, rank, PLACE_THERE)],
        [
            pltpu.VMEM((4, seq, rank), jnp.float32),
            pltpu.VMEM((tokens, rank), jnp.bfloat16),
            pltpu.VMEM((16, tall_b, rank), jnp.float32),
        ],
        rank,
        "backward_b",
    )
    came_b = core(send_b)

    def step_on(parts, axis, partner, k=0):
        leaving = functools.reduce(jnp.add, [part[k] for part in parts])
        rest = [part[1 - k] for part in parts]
        return [*rest, swap(leaving, axis, partner)]

    p = step_on([keep_p, came_p], X, first)
    w = step_on([keep_b, came_b], Z, first)
    p = step_on(p, Z, first)
    w = step_on(w, X, first)

    def both(k):
        p_sum, w_sum = (functools.reduce(jnp.add, [part[k] for part in parts]) for parts in (p, w))
        return jnp.concatenate([p_sum, w_sum], axis=-2)

    came = swap(both(1), X, second)
    shard = both(0) + came
    shard = shard[:2] + swap(shard[2:], Z, second)
    parts = (shard[0], swap(shard[1], Z, third))

    target = lax.dynamic_index_in_dim(pair_destination, place, 1, keepdims=False)
    hits = jnp.arange(pairs)[:, None] == target[None, :]
    moved = jnp.where(hits, margin[None, :] / ways, 0.0)
    loss = jnp.sum(jax.nn.softplus(-margin)) / (micro * pairs * ways)
    plain = jnp.broadcast_to(jnp.stack([jnp.zeros_like(loss), loss])[None], (pairs, 2))
    base = jnp.concatenate([moved, plain], axis=1)
    base = jnp.broadcast_to(base[:, None], (pairs, ways, micro + 2))
    base = base.reshape(pairs * ways, micro + 2)
    little = pltpu.CompilerParams(vmem_limit_bytes=4 * 2**20)
    f32 = lambda *shape: jax.ShapeDtypeStruct(shape, jnp.float32)
    shard, small = pl.pallas_call(
        pack_kernel, out_shape=[f32(*parts[0].shape), f32(*base.shape)], compiler_params=little
    )(*parts, base)
    small = lax.all_to_all(small, (X, Z, C, Y), 0, 0, tiled=True)
    grad_a, grad_b, pair_margin, mean_loss = pl.pallas_call(
        functools.partial(scale_kernel, (ff + width) * ways * rank),
        out_shape=[f32(tall_a, rank), f32(tall_b, rank), f32(micro, 1), f32(1, 1)],
        compiler_params=little,
    )(small, shard)
    return (pair_margin, mean_loss[0, 0], grad_a, grad_b)


def solution(mesh):
    split = Mesh(mesh.devices.reshape(4, 8, 2, mesh.shape["mp"]), (X, Z, C, Y))
    placed = (
        P(None, DP, None, None, Y),
        P(None, DP, None, None, Y),
        P(None, DP, None, None),
        P(None, DP, None, None),
        P(None, DP, None),
        P(),
        P(Y, None),
        P(Y, None),
    )

    return jax.shard_map(
        per_device,
        mesh=split,
        in_specs=placed,
        out_specs=(P(None, DP), P(), P(MP_DP, None), P(MP_DP, None)),
        check_vma=False,
    )
```
